64 devices in a mesh: data: 4 (over x, y), dap: 16 (over z, core).
Axes of the slice: x: 2, y: 2, z: 8, core: 2. Of those that a mesh axis runs over, the one named last changes fastest.
The devices are a block of a 4x4x8 slice.
Arguments:
- pair_act: bfloat16 [2048, 512, 128], P(('data', 'dap')), parts along dimension 0
- pair_mask: int32 [2048, 512], P(('data', 'dap')), parts along dimension 0
- d_pair_out: bfloat16 [2048, 512, 128], P(('data', 'dap')), parts along dimension 0
- ln_pair: bfloat16 [2, 2, 128], replicated
- w_proj: bfloat16 [2, 128, 512], replicated
- w_gate: bfloat16 [2, 128, 128], replicated
- ln_chan: bfloat16 [2, 2, 128], replicated
- w_out: bfloat16 [2, 128, 128], replicated
Outputs:
- output 1: bfloat16 [2048, 512, 128], P(('data', 'dap')), parts along dimension 0
- output 2: bfloat16 [2048, 512, 128], P(('data', 'dap')), parts along dimension 0
- output 3: bfloat16 [8, 2, 128], P('data'), parts along dimension 0
- output 4: bfloat16 [8, 128, 512], P('data'), parts along dimension 0
- output 5: bfloat16 [8, 128, 128], P('data'), parts along dimension 0
- output 6: bfloat16 [8, 2, 128], P('data'), parts along dimension 0
- output 7: bfloat16 [8, 128, 128], P('data'), parts along dimension 0
There are 4 independent parts. The reference program is written for one: setup_inputs(seed, part) draws one part's arguments, and reference() takes and returns one part's arrays. A program takes and returns all parts, laid end to end along the dimension named above; an argument that names none is the same for every part.
All inputs are finite; a program needn't handle non-finite values.
Results may differ from the reference program's by a relative error of at most 0.02.
Values are sent between devices in bfloat16 or wider.
A program may use at most 768 MiB of HBM per device.

```python
import jax
import jax.numpy as jnp
from jax import lax

N = 512
CZ = 128
CH = 128
LN_EPS = 1e-5


def layer_norm(values, gain_vec, shift_vec, norm_axis):
    mean_val = jnp.mean(values, axis=norm_axis, keepdims=True)
    centered = values - mean_val
    variance = jnp.mean(centered * centered, axis=norm_axis, keepdims=True)
    return centered * lax.rsqrt(variance + LN_EPS) * gain_vec + shift_vec


def draw_mask(mask_key):
    key_row, key_col, key_rhole, key_chole = jax.random.split(mask_key, 4)
    row_keep = jax.random.randint(key_row, (N,), 0, 25) != 0
    col_keep = jax.random.randint(key_col, (N,), 0, 25) != 0
    row_index = jnp.arange(N)
    row_keep = row_keep & (row_index != jax.random.randint(key_rhole, (), 0, N))
    col_keep = col_keep & (row_index != jax.random.randint(key_chole, (), 0, N))
    return (row_keep[:, None] & col_keep[None, :]).astype(jnp.int32)


def setup_inputs(seed: int = 0, part: int = 0) -> dict:
    part_key = jax.random.fold_in(jax.random.key(seed), part)
    key_act, key_grad, key_mask = jax.random.split(part_key, 3)
    shared = jax.random.split(jax.random.key(seed + 1), 7)
    pair_act = jax.random.normal(key_act, (N, N, CZ), jnp.float32).astype(jnp.bfloat16)
    d_pair_out = jax.random.normal(key_grad, (N, N, CZ), jnp.float32).astype(jnp.bfloat16)
    pair_mask = draw_mask(key_mask)
    ln_pair = jnp.stack([1.0 + 0.3 * jax.random.normal(shared[0], (2, CZ), jnp.float32), 0.3 * jax.random.normal(shared[1], (2, CZ), jnp.float32)], axis=1).astype(jnp.bfloat16)
    w_proj = (jax.random.normal(shared[2], (2, CZ, 4 * CH), jnp.float32) * CZ ** -0.5).astype(jnp.bfloat16)
    w_gate = (jax.random.normal(shared[3], (2, CZ, CZ), jnp.float32) * CZ ** -0.5).astype(jnp.bfloat16)
    ln_chan = jnp.stack([1.0 + 0.3 * jax.random.normal(shared[4], (2, CH), jnp.float32), 0.3 * jax.random.normal(shared[5], (2, CH), jnp.float32)], axis=1).astype(jnp.bfloat16)
    w_out = (jax.random.normal(shared[6], (2, CH, CZ), jnp.float32) * CH ** -0.5).astype(jnp.bfloat16)
    return {'pair_act': pair_act, 'pair_mask': pair_mask, 'd_pair_out': d_pair_out, 'ln_pair': ln_pair, 'w_proj': w_proj, 'w_gate': w_gate, 'ln_chan': ln_chan, 'w_out': w_out}


def project_rows(z_rows, mask_rows, ln_p, w_proj, w_gate):
    x_norm = layer_norm(z_rows, ln_p[0], ln_p[1], -1).astype(jnp.bfloat16).astype(jnp.float32)
    proj_all = jnp.einsum('ijd,de->eij', x_norm, w_proj)
    gate_val = jax.nn.sigmoid(jnp.einsum('ijd,de->ije', x_norm, w_gate))
    lin_a, pre_ga, lin_b, pre_gb = jnp.split(proj_all, 4, axis=0)
    mask_f = mask_rows.astype(jnp.float32)
    left_proj = (mask_f * jax.nn.sigmoid(pre_ga) * lin_a).astype(jnp.bfloat16)
    right_proj = (mask_f * jax.nn.sigmoid(pre_gb) * lin_b).astype(jnp.bfloat16)
    return left_proj, right_proj, gate_val


def tri_outgoing(left_grp, right_grp):
    return jnp.einsum('cik,cjk->cij', left_grp.astype(jnp.float32), right_grp.astype(jnp.float32)).astype(jnp.bfloat16)


def tri_incoming(left_grp, right_grp):
    return jnp.einsum('cki,ckj->cij', left_grp.astype(jnp.float32), right_grp.astype(jnp.float32)).astype(jnp.bfloat16)


def finish_rows(z_rows, t_rows, gate_val, ln_q, w_out):
    y_norm = layer_norm(t_rows.astype(jnp.float32), ln_q[0][:, None, None], ln_q[1][:, None, None], 0).astype(jnp.bfloat16).astype(jnp.float32)
    update_f = jnp.einsum('cij,cd->ijd', y_norm, w_out)
    return (z_rows + gate_val * update_f).astype(jnp.bfloat16)


def tri_update(z_pair, pair_mask, ln_p, w_proj, w_gate, ln_q, w_out, incoming):
    z_blocks = z_pair.astype(jnp.float32).reshape(N // 8, 8, N, CZ)
    mask_blocks = pair_mask.reshape(N // 8, 8, N)
    prep_fn = jax.checkpoint(project_rows)
    left_blk, right_blk, gate_blk = lax.map(lambda block_in: prep_fn(block_in[0], block_in[1], ln_p, w_proj, w_gate), (z_blocks, mask_blocks))
    left_groups = jnp.swapaxes(left_blk, 0, 1).reshape(8, CH // 8, N, N)
    right_groups = jnp.swapaxes(right_blk, 0, 1).reshape(8, CH // 8, N, N)
    tri_fn = jax.checkpoint(tri_incoming if incoming else tri_outgoing)
    t_groups = lax.map(lambda block_in: tri_fn(block_in[0], block_in[1]), (left_groups, right_groups))
    t_blocks = jnp.swapaxes(t_groups.reshape(CH, N // 8, 8, N), 0, 1)
    post_fn = jax.checkpoint(finish_rows)
    out_blocks = lax.map(lambda block_in: post_fn(block_in[0], block_in[1], block_in[2], ln_q, w_out), (z_blocks, t_blocks, gate_blk))
    return out_blocks.reshape(N, N, CZ)


def reference(pair_act, pair_mask, d_pair_out, ln_pair, w_proj, w_gate, ln_chan, w_out):
    def forward(z_in, ln_pair_in, w_proj_in, w_gate_in, ln_chan_in, w_out_in):
        ln_pf = ln_pair_in.astype(jnp.float32)
        proj_f = w_proj_in.astype(jnp.float32)
        gate_f = w_gate_in.astype(jnp.float32)
        ln_qf = ln_chan_in.astype(jnp.float32)
        out_f = w_out_in.astype(jnp.float32)
        z_mid = tri_update(z_in, pair_mask, ln_pf[0], proj_f[0], gate_f[0], ln_qf[0], out_f[0], False)
        return tri_update(z_mid, pair_mask, ln_pf[1], proj_f[1], gate_f[1], ln_qf[1], out_f[1], True)
    pair_out, pull_back = jax.vjp(forward, pair_act, ln_pair, w_proj, w_gate, ln_chan, w_out)
    d_pair, d_ln_p, d_w_p, d_w_g, d_ln_q, d_w_o = pull_back(d_pair_out)
    return pair_out, d_pair, d_ln_p, d_w_p, d_w_g, d_ln_q, d_w_o
```

```python
import functools

import jax
import jax.numpy as jnp
from jax import lax
from jax.experimental import pallas as pl
from jax.experimental.pallas import tpu as pltpu
from jax.sharding import PartitionSpec as P

LN_EPS = 1e-5
AXIS = 'dap'
F32 = jnp.float32
BF16 = jnp.bfloat16
RB = 16
KB = 256
MESH_ID = pl.DeviceIdType.MESH
ANY = pl.BlockSpec(memory_space=pl.ANY)
VM = pl.BlockSpec(memory_space=pltpu.VMEM)


def dot(lhs, rhs, lc, rc):
    return lax.dot_general(lhs, rhs, (((lc,), (rc,)), ((), ())), preferred_element_type=F32)


def norm(values, axis):
    mean = jnp.mean(values, axis=axis, keepdims=True)
    cent = values - mean
    var = jnp.mean(cent * cent, axis=axis, keepdims=True)
    rstd = lax.rsqrt(var + LN_EPS)
    return cent * rstd, rstd


def enter(n):
    me = lax.axis_index(AXIS)
    bar = pltpu.get_barrier_semaphore()

    def greet(s, carry):
        pl.semaphore_signal(bar, inc=1, device_id={AXIS: lax.rem(me + s, n)}, device_id_type=MESH_ID)
        return carry

    lax.fori_loop(1, n, greet, 0)
    pl.semaphore_wait(bar, n - 1)
    return me


def scatter(n, me, src, dst, ssem, rsem):
    def one(s, carry):
        peer = lax.rem(me + s, n)
        pltpu.make_async_remote_copy(src_ref=src(peer), dst_ref=dst(me), send_sem=ssem, recv_sem=rsem, device_id={AXIS: peer}, device_id_type=MESH_ID).start()
        return carry

    lax.fori_loop(1, n, one, 0)


def drain(ref, sem):
    pltpu.make_async_copy(ref, ref, sem).wait()


def block(q, n_cols):
    per = n_cols // KB
    i0 = pl.multiple_of((q // per) * RB, RB)
    k0 = pl.multiple_of(lax.rem(q, per) * KB, KB)
    return pl.ds(i0, RB), pl.ds(k0, KB), i0


def pack(s_ref, e0, count, write):
    def one(e, carry):
        off = pl.multiple_of(e * 8, 8)
        val = s_ref[:, pl.ds(e0 + off, 8), :]
        write(pl.ds(off, 8), jnp.swapaxes(val, 0, 1).astype(BF16))
        return carry

    lax.fori_loop(0, count // 8, one, 0)


def unpack(read, count, write):
    def one(e, carry):
        sl = pl.ds(pl.multiple_of(e * 16, 16), 16)
        write(sl, jnp.swapaxes(read(sl).astype(F32), 0, 1).astype(BF16))
        return carry

    lax.fori_loop(0, count // 16, one, 0)


def project(s_ref, i, x_row, m_row, wpt_ref, c):
    p = dot(wpt_ref[...], x_row, 1, 1)
    s_ref[i, 0:c, :] = m_row * jax.nn.sigmoid(p[c:2 * c]) * p[0:c]
    s_ref[i, c:2 * c, :] = m_row * jax.nn.sigmoid(p[3 * c:]) * p[2 * c:3 * c]


def fold_rows(v):
    return jnp.sum(v.reshape(v.shape[0] // 8, 8, v.shape[1]), axis=0)


def fold_lanes(v):
    out = v[:, 0:128]
    for h in range(1, v.shape[1] // 128):
        out = out + v[:, h * 128:(h + 1) * 128]
    return out


def send_ab(n, me, q, ri, rk, ab_send, ab_chan, rows, cl, sems):
    ssem, rsem, lsem = sems
    mine = pl.ds(me * rows, rows)
    row0 = me * rows

    def src(peer):
        return ab_send.at[:, pl.ds(peer * cl, cl), ri, rk]

    def dst(dev):
        return ab_chan.at[:, :, pl.ds(pl.multiple_of(dev * rows + ri.start, RB), RB), rk]

    pltpu.make_async_copy(src(me), dst(me), lsem).start()
    scatter(n, me, src, dst, ssem.at[q], rsem.at[q])


def finish_ab(n, nq, ab_send, ab_chan, rows, cl, sems):
    ssem, rsem, lsem = sems
    whole = ab_chan.at[:, :, pl.ds(0, rows), :]
    drain(whole, lsem)
    part = ab_chan.at[:, :, pl.ds(0, RB * (n - 1)), pl.ds(0, KB)]

    def one(q, carry):
        drain(part, ssem.at[q])
        drain(part, rsem.at[q])
        return carry

    lax.fori_loop(0, nq, one, 0)


def first_kernel(n, z_hbm, m_ref, gp_ref, wpt_ref, x_out, ab_chan, z_v, x_v, ab_send, s_ref, isem, osem, ssem, rsem, lsem):
    rows, cols, c = z_v.shape
    cl = c // n
    nq = (rows // RB) * (cols // KB)
    load = pltpu.make_async_copy(z_hbm, z_v, isem)
    load.start()
    me = enter(n)
    load.wait()
    sems = (ssem, rsem, lsem)

    def step(q, carry):
        ri, rk, i0 = block(q, cols)

        def row(i, carry2):
            xh, _ = norm(z_v[i0 + i, rk, :].astype(F32), -1)
            x_row = (xh * gp_ref[0:1, :] + gp_ref[1:2, :]).astype(BF16)
            x_v[i0 + i, rk, :] = x_row
            project(s_ref, i, x_row, m_ref[pl.ds(i0 + i, 1), rk], wpt_ref, c)
            return carry2

        lax.fori_loop(0, RB, row, 0)
        for h in range(2):
            def write(sl, val, h=h):
                ab_send[h, sl, ri, rk] = val
            pack(s_ref, h * c, c, write)
        send_ab(n, me, q, ri, rk, ab_send, ab_chan, rows, cl, sems)
        pltpu.make_async_copy(x_v.at[ri, rk, :], x_out.at[ri, rk, :], osem).start()
        return carry

    lax.fori_loop(0, nq, step, 0)
    drain(x_v, osem)
    finish_ab(n, nq, ab_send, ab_chan, rows, cl, sems)


def send_t(n, me, nq, cols, t_send, t_recv, rows, cl, ssem, rsem):
    def one(q, carry):
        ri, rk, i0 = block(q, cols)

        def src(peer):
            return t_send.at[:, pl.ds(pl.multiple_of(peer * rows + i0, RB), RB), rk]

        def dst(dev):
            return t_recv.at[pl.ds(dev * cl, cl), ri, rk]

        scatter(n, me, src, dst, ssem.at[q], rsem.at[q])
        return carry

    lax.fori_loop(0, nq, one, 0)

    def own(k, carry):
        t_recv[me * cl + k, :, :] = t_send[k, pl.ds(pl.multiple_of(me * rows, RB), rows), :]
        return carry

    lax.fori_loop(0, cl, own, 0)


def mid_kernel(n, ab_hbm, z_hbm, x_hbm, m_ref, gq_ref, wo_ref, wg_ref, gp_ref, wpt_ref,
               z_out, x_out, t_out, ab_chan,
               ab_v, z_v, x_v, t_send, t_recv, t_v, ab_send, s_ref, isem, osem, tss, trs, ssem, rsem, lsem):
    rows, cols, c = z_v.shape
    cl = c // n
    nq = (rows // RB) * (cols // KB)
    loads = [pltpu.make_async_copy(a, b, isem.at[k]) for k, (a, b) in enumerate(((ab_hbm, ab_v), (z_hbm, z_v), (x_hbm, x_v)))]
    for ld in loads:
        ld.start()
    me = enter(n)
    loads[0].wait()

    def tri(k, carry):
        t_send[k, :, :] = dot(ab_v[0, k], ab_v[1, k], 1, 1).astype(BF16)
        return carry

    lax.fori_loop(0, cl, tri, 0)
    send_t(n, me, nq, cols, t_send, t_recv, rows, cl, tss, trs)
    loads[1].wait()
    loads[2].wait()
    sems = (ssem, rsem, lsem)

    def step(q, carry):
        ri, rk, i0 = block(q, cols)
        drain(t_recv.at[pl.ds(0, c - cl), ri, rk], trs.at[q])

        def write_t(sl, val):
            t_v[ri, sl, rk] = val

        unpack(lambda sl: t_recv[sl, ri, rk], c, write_t)

        def row(i, carry2):
            r = i0 + i
            th, _ = norm(t_v[r, :, rk].astype(F32), 0)
            y = (th * gq_ref[0] + gq_ref[1]).astype(BF16)
            upd = dot(y, wo_ref[...], 0, 0)
            gate = jax.nn.sigmoid(dot(x_v[r, rk, :], wg_ref[...], 1, 0))
            z_new = (z_v[r, rk, :].astype(F32) + gate * upd).astype(BF16)
            z_v[r, rk, :] = z_new
            xh, _ = norm(z_new.astype(F32), -1)
            x_row = (xh * gp_ref[0:1, :] + gp_ref[1:2, :]).astype(BF16)
            x_v[r, rk, :] = x_row
            project(s_ref, i, x_row, m_ref[pl.ds(r, 1), rk], wpt_ref, c)
            return carry2

        lax.fori_loop(0, RB, row, 0)
        for h in range(2):
            def write(sl, val, h=h):
                ab_send[h, sl, ri, rk] = val
            pack(s_ref, h * c, c, write)
        send_ab(n, me, q, ri, rk, ab_send, ab_chan, rows, cl, sems)
        pltpu.make_async_copy(z_v.at[ri, rk, :], z_out.at[ri, rk, :], osem.at[0]).start()
        pltpu.make_async_copy(x_v.at[ri, rk, :], x_out.at[ri, rk, :], osem.at[1]).start()
        pltpu.make_async_copy(t_v.at[ri, :, rk], t_out.at[ri, :, rk], osem.at[2]).start()
        return carry

    lax.fori_loop(0, nq, step, 0)
    drain(z_v, osem.at[0])
    drain(x_v, osem.at[1])
    drain(t_v, osem.at[2])

    def sent(q, carry):
        drain(t_recv.at[pl.ds(0, c - cl), pl.ds(0, RB), pl.ds(0, KB)], tss.at[q])
        return carry

    lax.fori_loop(0, nq, sent, 0)
    finish_ab(n, nq, ab_send, ab_chan, rows, cl, sems)


def finish_back(i, r, rk, dn, th, rstd, y, upd, gate, gq_ref, wo_ref, dg_v, s_ref, gwo_ref, glq_ref):
    d_gate = dn * upd * gate * (1.0 - gate)
    d_upd = (dn * gate).astype(BF16)
    dg_v[r, rk, :] = d_gate.astype(BF16)
    gwo_ref[...] += dot(y, d_upd, 1, 0)
    dy = dot(wo_ref[...], d_upd, 1, 1).astype(BF16).astype(F32)
    glq_ref[0] += fold_lanes(dy * th)
    glq_ref[1] += fold_lanes(dy)
    dyg = dy * gq_ref[0]
    m1 = jnp.mean(dyg, axis=0, keepdims=True)
    m2 = jnp.mean(dyg * th, axis=0, keepdims=True)
    s_ref[i] = rstd * (dyg - m1 - th * m2)


def send_dt(n, me, q, ri, rk, dt_send, dt_chan, rows, cl, sems):
    ssem, rsem, lsem = sems

    def src(peer):
        return dt_send.at[pl.ds(peer * cl, cl), ri, rk]

    def dst(dev):
        return dt_chan.at[:, pl.ds(pl.multiple_of(dev * rows + ri.start, RB), RB), rk]

    pltpu.make_async_copy(src(me), dst(me), lsem).start()
    scatter(n, me, src, dst, ssem.at[q], rsem.at[q])


def finish_dt(n, nq, dt_chan, rows, sems):
    ssem, rsem, lsem = sems
    drain(dt_chan.at[:, pl.ds(0, rows), :], lsem)
    part = dt_chan.at[:, pl.ds(0, RB * (n - 1)), pl.ds(0, KB)]

    def one(q, carry):
        drain(part, ssem.at[q])
        drain(part, rsem.at[q])
        return carry

    lax.fori_loop(0, nq, one, 0)


def turn_kernel(n, ab_hbm, z_hbm, x_hbm, g_hbm, gq_ref, wo_ref, wg_ref,
                z_out, dg_out, dt_chan, gwo_ref, glq_ref,
                ab_v, z_v, x_v, g_v, dg_v, t_send, t_recv, t_v, dt_send, s_ref, isem, osem, tss, trs, ssem, rsem, lsem):
    rows, cols, c = z_v.shape
    cl = c // n
    nq = (rows // RB) * (cols // KB)
    loads = [pltpu.make_async_copy(a, b, isem.at[k]) for k, (a, b) in enumerate(((ab_hbm, ab_v), (z_hbm, z_v), (x_hbm, x_v), (g_hbm, g_v)))]
    for ld in loads:
        ld.start()
    gwo_ref[...] = jnp.zeros_like(gwo_ref)
    glq_ref[...] = jnp.zeros_like(glq_ref)
    me = enter(n)
    loads[0].wait()

    def tri(k, carry):
        t_send[k, :, :] = dot(ab_v[0, k], ab_v[1, k], 0, 0).astype(BF16)
        return carry

    lax.fori_loop(0, cl, tri, 0)
    send_t(n, me, nq, cols, t_send, t_recv, rows, cl, tss, trs)
    for ld in loads[1:]:
        ld.wait()
    sems = (ssem, rsem, lsem)

    def step(q, carry):
        ri, rk, i0 = block(q, cols)
        drain(t_recv.at[pl.ds(0, c - cl), ri, rk], trs.at[q])

        def write_t(sl, val):
            t_v[:, sl, :] = val

        unpack(lambda sl: t_recv[sl, ri, rk], c, write_t)

        def row(i, carry2):
            r = i0 + i
            th, rstd = norm(t_v[i].astype(F32), 0)
            y = (th * gq_ref[0] + gq_ref[1]).astype(BF16)
            upd = dot(y, wo_ref[...], 0, 0)
            gate = jax.nn.sigmoid(dot(x_v[r, rk, :], wg_ref[...], 1, 0))
            z_v[r, rk, :] = (z_v[r, rk, :].astype(F32) + gate * upd).astype(BF16)
            finish_back(i, r, rk, g_v[r, rk, :].astype(F32), th, rstd, y, upd, gate, gq_ref, wo_ref, dg_v, s_ref, gwo_ref, glq_ref)
            return carry2

        lax.fori_loop(0, RB, row, 0)

        def write(sl, val):
            dt_send[sl, ri, rk] = val

        pack(s_ref, 0, c, write)
        send_dt(n, me, q, ri, rk, dt_send, dt_chan, rows, cl, sems)
        pltpu.make_async_copy(z_v.at[ri, rk, :], z_out.at[ri, rk, :], osem.at[0]).start()
        pltpu.make_async_copy(dg_v.at[ri, rk, :], dg_out.at[ri, rk, :], osem.at[1]).start()
        return carry

    lax.fori_loop(0, nq, step, 0)
    drain(z_v, osem.at[0])
    drain(dg_v, osem.at[1])

    def sent(q, carry):
        drain(t_recv.at[pl.ds(0, c - cl), pl.ds(0, RB), pl.ds(0, KB)], tss.at[q])
        return carry

    lax.fori_loop(0, nq, sent, 0)
    finish_dt(n, nq, dt_chan, rows, sems)


def send_dab(n, me, nq, cols, ab_v, dab_recv, rows, cl, ssem, rsem):
    def one(q, carry):
        ri, rk, i0 = block(q, cols)

        def src(peer):
            return ab_v.at[:, :, pl.ds(pl.multiple_of(peer * rows + i0, RB), RB), rk]

        def dst(dev):
            return dab_recv.at[:, pl.ds(dev * cl, cl), ri, rk]

        scatter(n, me, src, dst, ssem.at[q], rsem.at[q])
        return carry

    lax.fori_loop(0, nq, one, 0)

    def own(k, carry):
        for h in range(2):
            dab_recv[h, me * cl + k, :, :] = ab_v[h, k, pl.ds(pl.multiple_of(me * rows, RB), rows), :]
        return carry

    lax.fori_loop(0, cl, own, 0)


def tri_back(cl, incoming, ab_v, dt_v):
    def one(k, carry):
        left, right, dt = ab_v[0, k], ab_v[1, k], dt_v[k]
        if incoming:
            d_left = dot(right, dt, 1, 1)
            d_right = dot(left, dt, 1, 0)
        else:
            d_left = dot(dt, right, 1, 0)
            d_right = dot(dt, left, 0, 0)
        ab_v[0, k, :, :] = d_left.astype(BF16)
        ab_v[1, k, :, :] = d_right.astype(BF16)
        return carry

    lax.fori_loop(0, cl, one, 0)


def project_back(i, r, rk, dab_t, m_ref, x_v, z_v, dg_v, dn_v, gp_ref, wpt_ref, wp_ref, wg_ref, gwp_ref, gwg_ref, glp_ref, c):
    x_row = x_v[r, rk, :]
    m_row = m_ref[pl.ds(r, 1), rk]
    p = dot(wpt_ref[...], x_row, 1, 1)
    parts = []
    for h in range(2):
        d_val = dab_t[i, h * c:(h + 1) * c, :].astype(F32) * m_row
        lin = p[2 * h * c:(2 * h + 1) * c]
        sig = jax.nn.sigmoid(p[(2 * h + 1) * c:(2 * h + 2) * c])
        d_lin = d_val * sig
        parts.append(d_lin.astype(BF16))
        parts.append((d_lin * lin * (1.0 - sig)).astype(BF16))
    d_proj = jnp.concatenate(parts, axis=0)
    d_gate = dg_v[r, rk, :]
    gwp_ref[...] += dot(d_proj, x_row, 1, 0)
    gwg_ref[...] += dot(x_row, d_gate, 0, 0)
    dxt = dot(wp_ref[...], d_proj, 1, 0) + dot(wg_ref[...], d_gate, 1, 1)
    dx = dxt.T.astype(BF16).astype(F32)
    xh, rstd = norm(z_v[r, rk, :].astype(F32), -1)
    glp_ref[0] += fold_rows(dx * xh)
    glp_ref[1] += fold_rows(dx)
    dxg = dx * gp_ref[0:1, :]
    m1 = jnp.mean(dxg, axis=-1, keepdims=True)
    m2 = jnp.mean(dxg * xh, axis=-1, keepdims=True)
    return (dn_v[r, rk, :].astype(F32) + rstd * (dxg - m1 - xh * m2)).astype(BF16)


def back_kernel(n, ab_hbm, dt_hbm, z_hbm, x_hbm, dg_hbm, dn_hbm, t_hbm, xp_hbm, m_ref, gp_ref, wpt_ref, wp_ref, wg_ref, gq_ref, wo_ref, wgp_ref,
                dn_out, dg_out, dt_chan, gwp_ref, gwg_ref, glp_ref, gwo_ref, glq_ref,
                ab_v, dt_v, z_v, x_v, dg_v, dn_v, t_v, xp_v, dab_recv, dab_t, dt_send, s_ref, isem, osem, tss, trs, ssem, rsem, lsem):
    rows, cols, c = z_v.shape
    cl = c // n
    nq = (rows // RB) * (cols // KB)
    pairs = ((ab_hbm, ab_v), (dt_hbm, dt_v), (z_hbm, z_v), (x_hbm, x_v), (dg_hbm, dg_v), (dn_hbm, dn_v), (t_hbm, t_v), (xp_hbm, xp_v))
    loads = [pltpu.make_async_copy(a, b, isem.at[k]) for k, (a, b) in enumerate(pairs)]
    for ld in loads:
        ld.start()
    for ref in (gwp_ref, gwg_ref, glp_ref, gwo_ref, glq_ref):
        ref[...] = jnp.zeros_like(ref)
    me = enter(n)
    loads[0].wait()
    loads[1].wait()
    tri_back(cl, True, ab_v, dt_v)
    send_dab(n, me, nq, cols, ab_v, dab_recv, rows, cl, tss, trs)
    for ld in loads[2:]:
        ld.wait()
    sems = (ssem, rsem, lsem)

    def step(q, carry):
        ri, rk, i0 = block(q, cols)
        drain(dab_recv.at[:, pl.ds(0, c - cl), ri, rk], trs.at[q])
        for h in range(2):
            def write_t(sl, val, h=h):
                dab_t[:, pl.ds(pl.multiple_of(h * c + sl.start, 16), 16), :] = val
            unpack(lambda sl, h=h: dab_recv[h, sl, ri, rk], c, write_t)

        def row(i, carry2):
            r = i0 + i
            dn = project_back(i, r, rk, dab_t, m_ref, x_v, z_v, dg_v, dn_v, gp_ref, wpt_ref, wp_ref, wg_ref, gwp_ref, gwg_ref, glp_ref, c)
            dn_v[r, rk, :] = dn
            th, rstd = norm(t_v[r, :, rk].astype(F32), 0)
            y = (th * gq_ref[0] + gq_ref[1]).astype(BF16)
            upd = dot(y, wo_ref[...], 0, 0)
            gate = jax.nn.sigmoid(dot(xp_v[r, rk, :], wgp_ref[...], 1, 0))
            finish_back(i, r, rk, dn.astype(F32), th, rstd, y, upd, gate, gq_ref, wo_ref, dg_v, s_ref, gwo_ref, glq_ref)
            return carry2

        lax.fori_loop(0, RB, row, 0)

        def write(sl, val):
            dt_send[sl, ri, rk] = val

        pack(s_ref, 0, c, write)
        send_dt(n, me, q, ri, rk, dt_send, dt_chan, rows, cl, sems)
        pltpu.make_async_copy(dn_v.at[ri, rk, :], dn_out.at[ri, rk, :], osem.at[0]).start()
        pltpu.make_async_copy(dg_v.at[ri, rk, :], dg_out.at[ri, rk, :], osem.at[1]).start()
        return carry

    lax.fori_loop(0, nq, step, 0)
    drain(dn_v, osem.at[0])
    drain(dg_v, osem.at[1])

    def sent(q, carry):
        drain(dab_recv.at[:, pl.ds(0, c - cl), pl.ds(0, RB), pl.ds(0, KB)], tss.at[q])
        return carry

    lax.fori_loop(0, nq, sent, 0)
    finish_dt(n, nq, dt_chan, rows, sems)


def last_kernel(n, ab_hbm, dt_hbm, z_hbm, x_hbm, dg_hbm, dn_hbm, m_ref, gp_ref, wpt_ref, wp_ref, wg_ref,
                dn_out, gwp_ref, gwg_ref, glp_ref,
                ab_v, dt_v, z_v, x_v, dg_v, dn_v, dab_recv, dab_t, isem, osem, tss, trs):
    rows, cols, c = z_v.shape
    cl = c // n
    nq = (rows // RB) * (cols // KB)
    pairs = ((ab_hbm, ab_v), (dt_hbm, dt_v), (z_hbm, z_v), (x_hbm, x_v), (dg_hbm, dg_v), (dn_hbm, dn_v))
    loads = [pltpu.make_async_copy(a, b, isem.at[k]) for k, (a, b) in enumerate(pairs)]
    for ld in loads:
        ld.start()
    for ref in (gwp_ref, gwg_ref, glp_ref):
        ref[...] = jnp.zeros_like(ref)
    me = enter(n)
    loads[0].wait()
    loads[1].wait()
    tri_back(cl, False, ab_v, dt_v)
    send_dab(n, me, nq, cols, ab_v, dab_recv, rows, cl, tss, trs)
    for ld in loads[2:]:
        ld.wait()

    def step(q, carry):
        ri, rk, i0 = block(q, cols)
        drain(dab_recv.at[:, pl.ds(0, c - cl), ri, rk], trs.at[q])
        for h in range(2):
            def write_t(sl, val, h=h):
                dab_t[:, pl.ds(pl.multiple_of(h * c + sl.start, 16), 16), :] = val
            unpack(lambda sl, h=h: dab_recv[h, sl, ri, rk], c, write_t)

        def row(i, carry2):
            r = i0 + i
            dn_v[r, rk, :] = project_back(i, r, rk, dab_t, m_ref, x_v, z_v, dg_v, dn_v, gp_ref, wpt_ref, wp_ref, wg_ref, gwp_ref, gwg_ref, glp_ref, c)
            return carry2

        lax.fori_loop(0, RB, row, 0)
        pltpu.make_async_copy(dn_v.at[ri, rk, :], dn_out.at[ri, rk, :], osem).start()
        return carry

    lax.fori_loop(0, nq, step, 0)
    drain(dn_v, osem)

    def sent(q, carry):
        drain(dab_recv.at[:, pl.ds(0, c - cl), pl.ds(0, RB), pl.ds(0, KB)], tss.at[q])
        return carry

    lax.fori_loop(0, nq, sent, 0)


def solution(mesh):
    row_spec = P(('data', AXIS), None, None)
    mask_spec = P(('data', AXIS), None)
    grad_spec = P('data', None, None)
    n = mesh.shape[AXIS]

    def device_step(z0, pair_mask, g, ln_pair, w_proj, w_gate, ln_chan, w_out):
        rows, cols, c = z0.shape
        cl = c // n
        nq = (rows // RB) * (cols // KB)
        mask_f = pair_mask.astype(F32)
        gp = ln_pair.astype(F32)
        gq = jnp.broadcast_to(ln_chan.astype(F32)[:, :, :, None], (2, 2, c, KB))
        wpt = jnp.swapaxes(w_proj, 1, 2)
        row_t = jax.ShapeDtypeStruct((rows, cols, c), BF16)
        t_row = jax.ShapeDtypeStruct((rows, c, cols), BF16)
        ab_t = jax.ShapeDtypeStruct((2, cl, cols, cols), BF16)
        dt_t = jax.ShapeDtypeStruct((cl, cols, cols), BF16)
        vm = pltpu.VMEM
        row_v = vm((rows, cols, c), BF16)
        ab_v = vm((2, cl, cols, cols), BF16)
        ab_rows = vm((2, c, rows, cols), BF16)
        t_c = vm((cl, cols, cols), BF16)
        t_rows = vm((c, rows, cols), BF16)
        dma = pltpu.SemaphoreType.DMA
        sq = dma((nq,))

        def call(body, cid, ins, outs, scratch, name):
            return pl.pallas_call(
                functools.partial(body, n),
                out_shape=tuple(o[0] for o in outs),
                in_specs=[s for _, s in ins],
                out_specs=tuple(o[1] for o in outs),
                scratch_shapes=scratch,
                compiler_params=pltpu.CompilerParams(collective_id=cid, has_side_effects=True, vmem_limit_bytes=63 * 1024 * 1024),
                name=name,
            )(*[a for a, _ in ins])

        def f32_out(*shape):
            return (jax.ShapeDtypeStruct(shape, F32), VM)

        x0, ab0 = call(first_kernel, 1,
                       [(z0, ANY), (mask_f, VM), (gp[0], VM), (wpt[0], VM)],
                       [(row_t, ANY), (ab_t, ANY)],
                       [row_v, row_v, ab_rows, vm((RB, 2 * c, KB), F32), dma, dma, sq, sq, dma], 'first')
        z1, x1, t0, ab1 = call(mid_kernel, 2,
                               [(ab0, ANY), (z0, ANY), (x0, ANY), (mask_f, VM), (gq[0], VM), (w_out[0], VM), (w_gate[0], VM), (gp[1], VM), (wpt[1], VM)],
                               [(row_t, ANY), (row_t, ANY), (t_row, ANY), (ab_t, ANY)],
                               [ab_v, row_v, row_v, t_c, t_rows, vm((rows, c, cols), BF16), ab_rows, vm((RB, 2 * c, KB), F32), dma((3,)), dma((3,)), sq, sq, sq, sq, dma], 'mid')
        z2, dg1, dt1, gwo1, glq1 = call(turn_kernel, 3,
                                        [(ab1, ANY), (z1, ANY), (x1, ANY), (g, ANY), (gq[1], VM), (w_out[1], VM), (w_gate[1], VM)],
                                        [(row_t, ANY), (row_t, ANY), (dt_t, ANY), f32_out(c, c), f32_out(2, c, 128)],
                                        [ab_v, row_v, row_v, row_v, row_v, t_c, t_rows, vm((RB, c, KB), BF16), t_rows, vm((RB, c, KB), F32), dma((4,)), dma((2,)), sq, sq, sq, sq, dma], 'turn')
        dmid, dg0, dt0, gwp1, gwg1, glp1, gwo0, glq0 = call(back_kernel, 4,
                                                            [(ab1, ANY), (dt1, ANY), (z1, ANY), (x1, ANY), (dg1, ANY), (g, ANY), (t0, ANY), (x0, ANY), (mask_f, VM), (gp[1], VM), (wpt[1], VM), (w_proj[1], VM), (w_gate[1], VM), (gq[0], VM), (w_out[0], VM), (w_gate[0], VM)],
                                                            [(row_t, ANY), (row_t, ANY), (dt_t, ANY), f32_out(4 * c, c), f32_out(c, c), f32_out(2, 8, c), f32_out(c, c), f32_out(2, c, 128)],
                                                            [ab_v, t_c, row_v, row_v, row_v, row_v, vm((rows, c, cols), BF16), row_v, ab_rows, vm((RB, 2 * c, KB), BF16), t_rows, vm((RB, c, KB), F32), dma((8,)), dma((2,)), sq, sq, sq, sq, dma], 'back')
        dz, gwp0, gwg0, glp0 = call(last_kernel, 5,
                                    [(ab0, ANY), (dt0, ANY), (z0, ANY), (x0, ANY), (dg0, ANY), (dmid, ANY), (mask_f, VM), (gp[0], VM), (wpt[0], VM), (w_proj[0], VM), (w_gate[0], VM)],
                                    [(row_t, ANY), f32_out(4 * c, c), f32_out(c, c), f32_out(2, 8, c)],
                                    [ab_v, t_c, row_v, row_v, row_v, row_v, ab_rows, vm((RB, 2 * c, KB), BF16), dma((6,)), dma, sq, sq], 'last')
        local = (jnp.stack([glp0.sum(1), glp1.sum(1)]), jnp.stack([gwp0, gwp1]), jnp.stack([gwg0, gwg1]), jnp.stack([glq0.sum(2), glq1.sum(2)]), jnp.stack([gwo0, gwo1]))
        tot = lax.psum(local, AXIS)
        tot = (tot[0], jnp.swapaxes(tot[1], 1, 2)) + tuple(tot[2:])
        return (z2, dz) + tuple(v.astype(BF16) for v in tot)

    full = P()
    return jax.shard_map(device_step, mesh=mesh, in_specs=(row_spec, mask_spec, row_spec, full, full, full, full, full), out_specs=(row_spec, row_spec, grad_spec, grad_spec, grad_spec, grad_spec, grad_spec), check_vma=False)
```

```python
import functools

import jax
import jax.numpy as jnp
from jax import lax
from jax.experimental import pallas as pl
from jax.experimental.pallas import tpu as pltpu
from jax.sharding import PartitionSpec as P

LN_EPS = 1e-5
AXIS = 'dap'
F32 = jnp.float32
BF16 = jnp.bfloat16
RB = 16
KB = 256
KB_EDGE = 128
UNROLL = 2
MESH_ID = pl.DeviceIdType.MESH
ANY = pl.BlockSpec(memory_space=pl.ANY)
VM = pl.BlockSpec(memory_space=pltpu.VMEM)


def dot(lhs, rhs, lc, rc):
    return lax.dot_general(lhs, rhs, (((lc,), (rc,)), ((), ())), preferred_element_type=F32)


def norm(values, axis):
    mean = jnp.mean(values, axis=axis, keepdims=True)
    cent = values - mean
    var = jnp.mean(cent * cent, axis=axis, keepdims=True)
    rstd = lax.rsqrt(var + LN_EPS)
    return cent * rstd, rstd


def greet(n):
    me = lax.axis_index(AXIS)
    bar = pltpu.get_barrier_semaphore()

    def one(s, carry):
        pl.semaphore_signal(bar, inc=1, device_id={AXIS: lax.rem(me + s, n)}, device_id_type=MESH_ID)
        return carry

    lax.fori_loop(1, n, one, 0)
    return me


def meet(n):
    pl.semaphore_wait(pltpu.get_barrier_semaphore(), n - 1)


def scatter(n, me, src, dst, ssem, rsem):
    def one(s, carry):
        peer = lax.rem(me + s, n)
        pltpu.make_async_remote_copy(src_ref=src(peer), dst_ref=dst(me), send_sem=ssem, recv_sem=rsem, device_id={AXIS: peer}, device_id_type=MESH_ID).start()
        return carry

    lax.fori_loop(1, n, one, 0)


def drain(ref, sem):
    pltpu.make_async_copy(ref, ref, sem).wait()


def drain_all(nq, part, *sems):
    def one(q, carry):
        for sem in sems:
            drain(part, sem.at[q])
        return carry

    lax.fori_loop(0, nq, one, 0)


def block(q, cols, kb):
    per = cols // kb
    i0 = pl.multiple_of((q // per) * RB, RB)
    k0 = pl.multiple_of(lax.rem(q, per) * kb, kb)
    return pl.ds(i0, RB), pl.ds(k0, kb), i0


def pair_params(u, lnp_ref):
    return lnp_ref[u, 0:1, :].astype(F32), lnp_ref[u, 1:2, :].astype(F32)


def load_wpt(u, wp_ref, wpt_v):
    wpt_v[...] = wp_ref[u].astype(F32).T.astype(BF16)


def load_mask(m_ref, m_v):
    for r in range(m_v.shape[0]):
        m_v[r, 0:1, :] = m_ref[r:r + 1, :].astype(F32)


def load_chan(u, lnq_ref, gq_v):
    c = gq_v.shape[1]
    for h in range(2):
        row = lnq_ref[u, h:h + 1, :].astype(F32)
        col = jnp.broadcast_to(row, (128, c)).T
        for l in range(gq_v.shape[2] // 128):
            gq_v[h, :, l * 128:(l + 1) * 128] = col


def pack(s_ref, e0, count, write):
    def one(e, carry):
        off = pl.multiple_of(e * 8, 8)
        val = s_ref[:, pl.ds(e0 + off, 8), :]
        write(pl.ds(off, 8), jnp.swapaxes(val, 0, 1).astype(BF16))
        return carry

    lax.fori_loop(0, count // 8, one, 0)


def unpack(read, count, write):
    def one(e, carry):
        sl = pl.ds(pl.multiple_of(e * 16, 16), 16)
        write(sl, jnp.swapaxes(read(sl).astype(F32), 0, 1).astype(BF16))
        return carry

    lax.fori_loop(0, count // 16, one, 0)


def each_row(row):
    lax.fori_loop(0, RB, row, 0, unroll=UNROLL)


def project(s_ref, i, x_row, m_row, wpt_v, c):
    p = dot(wpt_v[...], x_row, 1, 1)
    s_ref[i, 0:c, :] = m_row * jax.nn.sigmoid(p[c:2 * c]) * p[0:c]
    s_ref[i, c:2 * c, :] = m_row * jax.nn.sigmoid(p[3 * c:]) * p[2 * c:3 * c]


def fold_rows(v):
    return jnp.sum(v.reshape(v.shape[0] // 8, 8, v.shape[1]), axis=0)


def fold_lanes(v):
    out = v[:, 0:128]
    for h in range(1, v.shape[1] // 128):
        out = out + v[:, h * 128:(h + 1) * 128]
    return out


def send_ab(n, me, q, ri, rk, ab_send, ab_chan, rows, cl, sems):
    ssem, rsem, lsem = sems

    def src(peer):
        return ab_send.at[:, pl.ds(peer * cl, cl), ri, rk]

    def dst(dev):
        return ab_chan.at[:, :, pl.ds(pl.multiple_of(dev * rows + ri.start, RB), RB), rk]

    pltpu.make_async_copy(src(me), dst(me), lsem).start()
    scatter(n, me, src, dst, ssem.at[q], rsem.at[q])


def finish_ab(n, nq, kb, ab_chan, rows, sems):
    ssem, rsem, lsem = sems
    drain(ab_chan.at[:, :, pl.ds(0, rows), :], lsem)
    drain_all(nq, ab_chan.at[:, :, pl.ds(0, RB * (n - 1)), pl.ds(0, kb)], ssem, rsem)


def pack_ab(s_ref, c, ab_send, ri, rk):
    for h in range(2):
        def write(sl, val, h=h):
            ab_send[h, sl, ri, rk] = val
        pack(s_ref, h * c, c, write)


def first_kernel(n, z_hbm, m_ref, lnp_ref, wp_ref, x_out, ab_chan, z_v, x_v, ab_send, s_ref, wpt_v, m_v, isem, osem, ssem, rsem, lsem):
    rows, cols, c = z_v.shape
    cl = c // n
    kb = KB_EDGE
    nq = (rows // RB) * (cols // kb)
    load = pltpu.make_async_copy(z_hbm, z_v, isem)
    load.start()
    me = greet(n)
    load_wpt(0, wp_ref, wpt_v)
    load_mask(m_ref, m_v)
    gain, shift = pair_params(0, lnp_ref)
    load.wait()
    sems = (ssem, rsem, lsem)

    def step(q, carry):
        ri, rk, i0 = block(q, cols, kb)

        def row(i, carry2):
            r = i0 + i
            xh, _ = norm(z_v[r, rk, :].astype(F32), -1)
            x_row = (xh * gain + shift).astype(BF16)
            x_v[r, rk, :] = x_row
            project(s_ref, i, x_row, m_v[r, 0:1, rk], wpt_v, c)
            return carry2

        each_row(row)
        pack_ab(s_ref, c, ab_send, ri, rk)

        @pl.when(q == 0)
        def _():
            meet(n)

        send_ab(n, me, q, ri, rk, ab_send, ab_chan, rows, cl, sems)
        pltpu.make_async_copy(x_v.at[ri, rk, :], x_out.at[ri, rk, :], osem).start()
        return carry

    lax.fori_loop(0, nq, step, 0)
    drain(x_v, osem)
    finish_ab(n, nq, kb, ab_chan, rows, sems)


def exchange_t(n, me, nq, cols, kb, product, t_send, t_recv, rows, cl, ssem, rsem):
    def send(k0, count, q):
        ri, rk, i0 = block(q, cols, kb)

        def src(peer):
            return t_send.at[pl.ds(k0, count), pl.ds(pl.multiple_of(peer * rows + i0, RB), RB), rk]

        def dst(dev):
            return t_recv.at[pl.ds(dev * cl + k0, count), ri, rk]

        scatter(n, me, src, dst, ssem.at[q], rsem.at[q])

    def one(k, carry):
        product(k)

        @pl.when(k == 0)
        def _():
            meet(n)

        send(k, 1, 0)
        return carry

    lax.fori_loop(0, cl, one, 0)

    def rest(q, carry):
        send(0, cl, q)
        return carry

    lax.fori_loop(1, nq, rest, 0)

    def own(k, carry):
        t_recv[me * cl + k, :, :] = t_send[k, pl.ds(pl.multiple_of(me * rows, RB), rows), :]
        return carry

    lax.fori_loop(0, cl, own, 0)


def start_loads(chan_pairs, row_pairs, csem, isem):
    cl = csem.shape[1]
    chan = []
    for h, (src, dst) in enumerate(chan_pairs):
        def cut(k, src=src, dst=dst, h=h):
            return pltpu.make_async_copy(src(k), dst(k), csem.at[h, k])
        chan.append(cut)

    def one(k, carry):
        for cut in chan:
            cut(k).start()
        return carry

    lax.fori_loop(0, cl, one, 0)
    loads = [pltpu.make_async_copy(a, b, isem.at[j]) for j, (a, b) in enumerate(row_pairs)]
    for ld in loads:
        ld.start()

    def wait_chan(k):
        for cut in chan:
            cut(k).wait()

    def wait_rows():
        for ld in loads:
            ld.wait()

    return wait_chan, wait_rows


def mid_kernel(n, ab_hbm, z_hbm, x_hbm, m_ref, lnp_ref, wp_ref, wg_ref, lnq_ref, wo_ref,
               z_out, x_out, t_out, ab_chan,
               ab_v, z_v, x_v, t_send, t_recv, t_v, ab_send, s_ref, wpt_v, m_v, gq_v, csem, isem, osem, tss, trs, ssem, rsem, lsem):
    rows, cols, c = z_v.shape
    cl = c // n
    kb = KB
    nq = (rows // RB) * (cols // kb)
    wait_chan, wait_rows = start_loads([(lambda k: ab_hbm.at[:, k], lambda k: ab_v.at[:, k])], [(z_hbm, z_v), (x_hbm, x_v)], csem, isem)
    me = greet(n)
    load_wpt(1, wp_ref, wpt_v)
    load_mask(m_ref, m_v)
    load_chan(0, lnq_ref, gq_v)
    gain, shift = pair_params(1, lnp_ref)

    def product(k):
        wait_chan(k)
        t_send[k, :, :] = dot(ab_v[0, k], ab_v[1, k], 1, 1).astype(BF16)

    exchange_t(n, me, nq, cols, kb, product, t_send, t_recv, rows, cl, tss, trs)
    wait_rows()
    sems = (ssem, rsem, lsem)

    def step(q, carry):
        ri, rk, i0 = block(q, cols, kb)
        drain(t_recv.at[pl.ds(0, c - cl), ri, rk], trs.at[q])

        def write_t(sl, val):
            t_v[ri, sl, rk] = val

        unpack(lambda sl: t_recv[sl, ri, rk], c, write_t)

        def row(i, carry2):
            r = i0 + i
            th, _ = norm(t_v[r, :, rk].astype(F32), 0)
            y = (th * gq_v[0] + gq_v[1]).astype(BF16)
            upd = dot(y, wo_ref[0], 0, 0)
            gate = jax.nn.sigmoid(dot(x_v[r, rk, :], wg_ref[0], 1, 0))
            z_new = (z_v[r, rk, :].astype(F32) + gate * upd).astype(BF16)
            z_v[r, rk, :] = z_new
            xh, _ = norm(z_new.astype(F32), -1)
            x_row = (xh * gain + shift).astype(BF16)
            x_v[r, rk, :] = x_row
            project(s_ref, i, x_row, m_v[r, 0:1, rk], wpt_v, c)
            return carry2

        each_row(row)
        pack_ab(s_ref, c, ab_send, ri, rk)
        send_ab(n, me, q, ri, rk, ab_send, ab_chan, rows, cl, sems)
        pltpu.make_async_copy(z_v.at[ri, rk, :], z_out.at[ri, rk, :], osem.at[0]).start()
        pltpu.make_async_copy(x_v.at[ri, rk, :], x_out.at[ri, rk, :], osem.at[1]).start()
        pltpu.make_async_copy(t_v.at[ri, :, rk], t_out.at[ri, :, rk], osem.at[2]).start()
        return carry

    lax.fori_loop(0, nq, step, 0)
    drain(z_v, osem.at[0])
    drain(x_v, osem.at[1])
    drain(t_v, osem.at[2])
    drain_all(nq, t_recv.at[pl.ds(0, c - cl), pl.ds(0, RB), pl.ds(0, kb)], tss)
    finish_ab(n, nq, kb, ab_chan, rows, sems)


def finish_back(i, r, rk, dn, th, rstd, y, upd, gate, gq_v, w_out, dg_v, s_ref, gwo_ref, glq_ref):
    d_gate = dn * upd * gate * (1.0 - gate)
    d_upd = (dn * gate).astype(BF16)
    dg_v[r, rk, :] = d_gate.astype(BF16)
    gwo_ref[...] += dot(y, d_upd, 1, 0)
    dy = dot(w_out, d_upd, 1, 1).astype(BF16).astype(F32)
    glq_ref[0] += fold_lanes(dy * th)
    glq_ref[1] += fold_lanes(dy)
    dyg = dy * gq_v[0]
    m1 = jnp.mean(dyg, axis=0, keepdims=True)
    m2 = jnp.mean(dyg * th, axis=0, keepdims=True)
    s_ref[i] = rstd * (dyg - m1 - th * m2)


def send_dt(n, me, q, ri, rk, dt_send, dt_chan, rows, cl, sems):
    ssem, rsem, lsem = sems

    def src(peer):
        return dt_send.at[pl.ds(peer * cl, cl), ri, rk]

    def dst(dev):
        return dt_chan.at[:, pl.ds(pl.multiple_of(dev * rows + ri.start, RB), RB), rk]

    pltpu.make_async_copy(src(me), dst(me), lsem).start()
    scatter(n, me, src, dst, ssem.at[q], rsem.at[q])


def finish_dt(n, nq, kb, dt_chan, rows, sems):
    ssem, rsem, lsem = sems
    drain(dt_chan.at[:, pl.ds(0, rows), :], lsem)
    drain_all(nq, dt_chan.at[:, pl.ds(0, RB * (n - 1)), pl.ds(0, kb)], ssem, rsem)


def turn_kernel(n, ab_hbm, z_hbm, x_hbm, g_hbm, wg_ref, lnq_ref, wo_ref,
                z_out, dg_out, dt_chan, gwo_ref, glq_ref,
                ab_v, z_v, x_v, g_v, dg_v, t_send, t_recv, t_v, dt_send, s_ref, gq_v, csem, isem, osem, tss, trs, ssem, rsem, lsem):
    rows, cols, c = z_v.shape
    cl = c // n
    kb = KB
    nq = (rows // RB) * (cols // kb)
    wait_chan, wait_rows = start_loads([(lambda k: ab_hbm.at[:, k], lambda k: ab_v.at[:, k])], [(z_hbm, z_v), (x_hbm, x_v), (g_hbm, g_v)], csem, isem)
    me = greet(n)
    gwo_ref[...] = jnp.zeros_like(gwo_ref)
    glq_ref[...] = jnp.zeros_like(glq_ref)
    load_chan(1, lnq_ref, gq_v)

    def product(k):
        wait_chan(k)
        t_send[k, :, :] = dot(ab_v[0, k], ab_v[1, k], 0, 0).astype(BF16)

    exchange_t(n, me, nq, cols, kb, product, t_send, t_recv, rows, cl, tss, trs)
    wait_rows()
    sems = (ssem, rsem, lsem)

    def step(q, carry):
        ri, rk, i0 = block(q, cols, kb)
        drain(t_recv.at[pl.ds(0, c - cl), ri, rk], trs.at[q])

        def write_t(sl, val):
            t_v[:, sl, :] = val

        unpack(lambda sl: t_recv[sl, ri, rk], c, write_t)

        def row(i, carry2):
            r = i0 + i
            th, rstd = norm(t_v[i].astype(F32), 0)
            y = (th * gq_v[0] + gq_v[1]).astype(BF16)
            upd = dot(y, wo_ref[1], 0, 0)
            gate = jax.nn.sigmoid(dot(x_v[r, rk, :], wg_ref[1], 1, 0))
            z_v[r, rk, :] = (z_v[r, rk, :].astype(F32) + gate * upd).astype(BF16)
            finish_back(i, r, rk, g_v[r, rk, :].astype(F32), th, rstd, y, upd, gate, gq_v, wo_ref[1], dg_v, s_ref, gwo_ref, glq_ref)
            return carry2

        each_row(row)

        def write(sl, val):
            dt_send[sl, ri, rk] = val

        pack(s_ref, 0, c, write)
        send_dt(n, me, q, ri, rk, dt_send, dt_chan, rows, cl, sems)
        pltpu.make_async_copy(z_v.at[ri, rk, :], z_out.at[ri, rk, :], osem.at[0]).start()
        pltpu.make_async_copy(dg_v.at[ri, rk, :], dg_out.at[ri, rk, :], osem.at[1]).start()
        return carry

    lax.fori_loop(0, nq, step, 0)
    drain(z_v, osem.at[0])
    drain(dg_v, osem.at[1])
    drain_all(nq, t_recv.at[pl.ds(0, c - cl), pl.ds(0, RB), pl.ds(0, kb)], tss)
    finish_dt(n, nq, kb, dt_chan, rows, sems)


def exchange_dab(n, me, nq, cols, kb, incoming, wait_chan, ab_v, dt_v, dab_recv, rows, cl, ssem, rsem, between):
    def send(k0, count, q):
        ri, rk, i0 = block(q, cols, kb)

        def src(peer):
            return ab_v.at[:, pl.ds(k0, count), pl.ds(pl.multiple_of(peer * rows + i0, RB), RB), rk]

        def dst(dev):
            return dab_recv.at[:, pl.ds(dev * cl + k0, count), ri, rk]

        scatter(n, me, src, dst, ssem.at[q], rsem.at[q])

    def one(k, carry):
        wait_chan(k)
        left, right, dt = ab_v[0, k], ab_v[1, k], dt_v[k]
        if incoming:
            d_left = dot(right, dt, 1, 1)
            d_right = dot(left, dt, 1, 0)
        else:
            d_left = dot(dt, right, 1, 0)
            d_right = dot(dt, left, 0, 0)
        ab_v[0, k, :, :] = d_left.astype(BF16)
        ab_v[1, k, :, :] = d_right.astype(BF16)

        @pl.when(k == 0)
        def _():
            between()

        send(k, 1, 0)
        return carry

    lax.fori_loop(0, cl, one, 0)

    def rest(q, carry):
        send(0, cl, q)
        return carry

    lax.fori_loop(1, nq, rest, 0)

    def own(k, carry):
        for h in range(2):
            dab_recv[h, me * cl + k, :, :] = ab_v[h, k, pl.ds(pl.multiple_of(me * rows, RB), rows), :]
        return carry

    lax.fori_loop(0, cl, own, 0)


def unpack_dab(dab_recv, dab_t, c, ri, rk):
    for h in range(2):
        def write_t(sl, val, h=h):
            dab_t[:, pl.ds(pl.multiple_of(h * c + sl.start, 16), 16), :] = val
        unpack(lambda sl, h=h: dab_recv[h, sl, ri, rk], c, write_t)


def project_back(u, i, r, rk, dab_t, m_v, x_v, z_v, dg_v, dn_v, gain, wpt_v, wp_ref, wg_ref, gwp_ref, gwg_ref, glp_ref, c):
    x_row = x_v[r, rk, :]
    m_row = m_v[r, 0:1, rk]
    p = dot(wpt_v[...], x_row, 1, 1)
    parts = []
    for h in range(2):
        d_val = dab_t[i, h * c:(h + 1) * c, :].astype(F32) * m_row
        lin = p[2 * h * c:(2 * h + 1) * c]
        sig = jax.nn.sigmoid(p[(2 * h + 1) * c:(2 * h + 2) * c])
        d_lin = d_val * sig
        parts.append(d_lin.astype(BF16))
        parts.append((d_lin * lin * (1.0 - sig)).astype(BF16))
    d_proj = jnp.concatenate(parts, axis=0)
    d_gate = dg_v[r, rk, :]
    gwp_ref[...] += dot(d_proj, x_row, 1, 0)
    gwg_ref[...] += dot(x_row, d_gate, 0, 0)
    dxt = dot(wp_ref[u], d_proj, 1, 0) + dot(wg_ref[u], d_gate, 1, 1)
    dx = dxt.T.astype(BF16).astype(F32)
    xh, rstd = norm(z_v[r, rk, :].astype(F32), -1)
    glp_ref[0] += fold_rows(dx * xh)
    glp_ref[1] += fold_rows(dx)
    dxg = dx * gain
    m1 = jnp.mean(dxg, axis=-1, keepdims=True)
    m2 = jnp.mean(dxg * xh, axis=-1, keepdims=True)
    return (dn_v[r, rk, :].astype(F32) + rstd * (dxg - m1 - xh * m2)).astype(BF16)


def back_kernel(n, ab_hbm, dt_hbm, z_hbm, x_hbm, dg_hbm, dn_hbm, t_hbm, xp_hbm, m_ref, lnp_ref, wp_ref, wg_ref, lnq_ref, wo_ref,
                dn_out, dg_out, dt_chan, gwp_ref, gwg_ref, glp_ref, gwo_ref, glq_ref,
                ab_v, dt_v, z_v, x_v, dg_v, dn_v, t_v, xp_v, dab_recv, dab_t, dt_send, s_ref, wpt_v, m_v, gq_v, csem, isem, osem, tss, trs, ssem, rsem, lsem):
    rows, cols, c = z_v.shape
    cl = c // n
    kb = KB
    nq = (rows // RB) * (cols // kb)
    chan = [(lambda k: ab_hbm.at[:, k], lambda k: ab_v.at[:, k]), (lambda k: dt_hbm.at[k], lambda k: dt_v.at[k])]
    wait_chan, wait_rows = start_loads(chan, [(z_hbm, z_v), (x_hbm, x_v), (dg_hbm, dg_v), (dn_hbm, dn_v), (t_hbm, t_v), (xp_hbm, xp_v)], csem, isem)
    me = greet(n)
    for ref in (gwp_ref, gwg_ref, glp_ref, gwo_ref, glq_ref):
        ref[...] = jnp.zeros_like(ref)
    load_wpt(1, wp_ref, wpt_v)
    load_mask(m_ref, m_v)
    load_chan(0, lnq_ref, gq_v)
    gain, _ = pair_params(1, lnp_ref)
    exchange_dab(n, me, nq, cols, kb, True, wait_chan, ab_v, dt_v, dab_recv, rows, cl, tss, trs, lambda: meet(n))
    wait_rows()
    sems = (ssem, rsem, lsem)

    def step(q, carry):
        ri, rk, i0 = block(q, cols, kb)
        drain(dab_recv.at[:, pl.ds(0, c - cl), ri, rk], trs.at[q])
        unpack_dab(dab_recv, dab_t, c, ri, rk)

        def row(i, carry2):
            r = i0 + i
            dn = project_back(1, i, r, rk, dab_t, m_v, x_v, z_v, dg_v, dn_v, gain, wpt_v, wp_ref, wg_ref, gwp_ref, gwg_ref, glp_ref, c)
            dn_v[r, rk, :] = dn
            th, rstd = norm(t_v[r, :, rk].astype(F32), 0)
            y = (th * gq_v[0] + gq_v[1]).astype(BF16)
            upd = dot(y, wo_ref[0], 0, 0)
            gate = jax.nn.sigmoid(dot(xp_v[r, rk, :], wg_ref[0], 1, 0))
            finish_back(i, r, rk, dn.astype(F32), th, rstd, y, upd, gate, gq_v, wo_ref[0], dg_v, s_ref, gwo_ref, glq_ref)
            return carry2

        each_row(row)

        def write(sl, val):
            dt_send[sl, ri, rk] = val

        pack(s_ref, 0, c, write)
        send_dt(n, me, q, ri, rk, dt_send, dt_chan, rows, cl, sems)
        pltpu.make_async_copy(dn_v.at[ri, rk, :], dn_out.at[ri, rk, :], osem.at[0]).start()
        pltpu.make_async_copy(dg_v.at[ri, rk, :], dg_out.at[ri, rk, :], osem.at[1]).start()
        return carry

    lax.fori_loop(0, nq, step, 0)
    drain(dn_v, osem.at[0])
    drain(dg_v, osem.at[1])
    drain_all(nq, dab_recv.at[:, pl.ds(0, c - cl), pl.ds(0, RB), pl.ds(0, kb)], tss)
    finish_dt(n, nq, kb, dt_chan, rows, sems)


def add_parts(n, recv):
    def one(s, acc):
        return acc + recv[s]

    return lax.fori_loop(1, n, one, recv[0])


def last_kernel(n, ab_hbm, dt_hbm, z_hbm, x_hbm, dg_hbm, dn_hbm, m_ref, lnp_ref, wp_ref, wg_ref,
                gwp1_ref, gwg1_ref, gwo1_ref, gwo0_ref, glp1_ref, glq1_ref, glq0_ref,
                dn_out, grads_out, small_out,
                ab_v, dt_v, z_v, x_v, dg_v, dn_v, dab_recv, dab_t, wpt_v, m_v, gwp_ref, gwg_ref, glp_ref, early, early_in, late, late_in, mine,
                csem, isem, osem, tss, trs, gss, grs, lsem):
    rows, cols, c = z_v.shape
    cl = c // n
    kb = KB_EDGE
    nq = (rows // RB) * (cols // kb)
    we, wc = 4 * c // n, c // n
    chan = [(lambda k: ab_hbm.at[:, k], lambda k: ab_v.at[:, k]), (lambda k: dt_hbm.at[k], lambda k: dt_v.at[k])]
    wait_chan, wait_rows = start_loads(chan, [(z_hbm, z_v), (x_hbm, x_v), (dg_hbm, dg_v), (dn_hbm, dn_v)], csem, isem)
    me = greet(n)
    for ref in (gwp_ref, gwg_ref, glp_ref):
        ref[...] = jnp.zeros_like(ref)
    load_wpt(0, wp_ref, wpt_v)
    load_mask(m_ref, m_v)
    gain, _ = pair_params(0, lnp_ref)
    small = [jnp.sum(glp1_ref[h], axis=0, keepdims=True) for h in range(2)]
    small += [jnp.sum(ref[h].T, axis=0, keepdims=True) for ref in (glq1_ref, glq0_ref) for h in range(2)]
    small = jnp.concatenate(small + [jnp.zeros((2, c), F32)], axis=0)
    e1, e2, e3, e4 = we, we + wc, we + 2 * wc, we + 3 * wc

    def fill(p, carry):
        early[p, 0:e1, :] = gwp1_ref[pl.ds(pl.multiple_of(p * we, 8), we), :]
        cut = pl.ds(pl.multiple_of(p * wc, 8), wc)
        early[p, e1:e2, :] = gwg1_ref[cut, :]
        early[p, e2:e3, :] = gwo1_ref[cut, :]
        early[p, e3:e4, :] = gwo0_ref[cut, :]
        early[p, e4:e4 + 8, :] = small
        return carry

    lax.fori_loop(0, n, fill, 0)
    early_in[me] = early[me]

    def between():
        meet(n)

    exchange_dab(n, me, nq, cols, kb, False, wait_chan, ab_v, dt_v, dab_recv, rows, cl, tss, trs, between)
    scatter(n, me, lambda p: early.at[p], lambda d: early_in.at[d], gss.at[0], grs.at[0])
    wait_rows()

    def step(q, carry):
        ri, rk, i0 = block(q, cols, kb)
        drain(dab_recv.at[:, pl.ds(0, c - cl), ri, rk], trs.at[q])
        unpack_dab(dab_recv, dab_t, c, ri, rk)

        def row(i, carry2):
            r = i0 + i
            dn_v[r, rk, :] = project_back(0, i, r, rk, dab_t, m_v, x_v, z_v, dg_v, dn_v, gain, wpt_v, wp_ref, wg_ref, gwp_ref, gwg_ref, glp_ref, c)
            return carry2

        each_row(row)
        pltpu.make_async_copy(dn_v.at[ri, rk, :], dn_out.at[ri, rk, :], osem).start()
        return carry

    lax.fori_loop(0, nq, step, 0)
    tail = jnp.concatenate([jnp.sum(glp_ref[h], axis=0, keepdims=True) for h in range(2)] + [jnp.zeros((6, c), F32)], axis=0)

    def fill_late(p, carry):
        late[p, 0:e1, :] = gwp_ref[pl.ds(pl.multiple_of(p * we, 8), we), :]
        late[p, e1:e2, :] = gwg_ref[pl.ds(pl.multiple_of(p * wc, 8), wc), :]
        late[p, e2:e2 + 8, :] = tail
        return carry

    lax.fori_loop(0, n, fill_late, 0)
    late_in[me] = late[me]
    scatter(n, me, lambda p: late.at[p], lambda d: late_in.at[d], gss.at[1], grs.at[1])
    part = early.at[pl.ds(0, n - 1)]
    drain(part, grs.at[0])
    sum_e = add_parts(n, early_in)
    part_l = late.at[pl.ds(0, n - 1)]
    drain(part_l, grs.at[1])
    sum_l = add_parts(n, late_in)
    mine[...] = jnp.concatenate([sum_e[0:e1], sum_l[0:e1], sum_e[e1:e4], sum_l[e1:e2]], axis=0).astype(BF16)
    small_out[0:8, :] = sum_e[e4:e4 + 8]
    small_out[8:16, :] = sum_l[e2:e2 + 8]
    own = pltpu.make_async_copy(mine, grads_out.at[me], lsem)
    own.start()
    scatter(n, me, lambda p: mine, lambda d: grads_out.at[d], gss.at[2], grs.at[2])
    drain(dn_v, osem)
    drain_all(nq, dab_recv.at[:, pl.ds(0, c - cl), pl.ds(0, RB), pl.ds(0, kb)], tss)
    drain(part, gss.at[0])
    drain(part_l, gss.at[1])
    own.wait()
    gathered = grads_out.at[pl.ds(0, n - 1)]
    drain(gathered, gss.at[2])
    drain(gathered, grs.at[2])


def solution(mesh):
    row_spec = P(('data', AXIS), None, None)
    mask_spec = P(('data', AXIS), None)
    grad_spec = P('data', None, None)
    n = mesh.shape[AXIS]

    def device_step(z0, mask, g, ln_pair, w_proj, w_gate, ln_chan, w_out):
        rows, cols, c = z0.shape
        cl = c // n
        nq = (rows // RB) * (cols // KB)
        ne = (rows // RB) * (cols // KB_EDGE)
        row_t = jax.ShapeDtypeStruct((rows, cols, c), BF16)
        t_row = jax.ShapeDtypeStruct((rows, c, cols), BF16)
        ab_t = jax.ShapeDtypeStruct((2, cl, cols, cols), BF16)
        dt_t = jax.ShapeDtypeStruct((cl, cols, cols), BF16)
        vm = pltpu.VMEM
        row_v = vm((rows, cols, c), BF16)
        ab_v = vm((2, cl, cols, cols), BF16)
        ab_rows = vm((2, c, rows, cols), BF16)
        t_c = vm((cl, cols, cols), BF16)
        t_rows = vm((c, rows, cols), BF16)
        wpt_v = vm((4 * c, c), BF16)
        gq_v = vm((2, c, KB), F32)
        m_v = vm((rows, 1, cols), F32)
        dma = pltpu.SemaphoreType.DMA
        sq, se = dma((nq,)), dma((ne,))

        def call(body, cid, ins, outs, scratch, name):
            return pl.pallas_call(
                functools.partial(body, n),
                out_shape=tuple(o[0] for o in outs),
                in_specs=[s for _, s in ins],
                out_specs=tuple(o[1] for o in outs),
                scratch_shapes=scratch,
                compiler_params=pltpu.CompilerParams(collective_id=cid, has_side_effects=True, vmem_limit_bytes=63 * 1024 * 1024),
                name=name,
            )(*[a for a, _ in ins])

        def f32_out(*shape):
            return (jax.ShapeDtypeStruct(shape, F32), VM)

        mk, lnp, wp, wg, lnq, wo = ((v, VM) for v in (mask, ln_pair, w_proj, w_gate, ln_chan, w_out))
        x0, ab0 = call(first_kernel, 1, [(z0, ANY), mk, lnp, wp], [(row_t, ANY), (ab_t, ANY)],
                       [row_v, row_v, ab_rows, vm((RB, 2 * c, KB_EDGE), F32), wpt_v, m_v, dma, dma, se, se, dma], 'first')
        z1, x1, t0, ab1 = call(mid_kernel, 2, [(ab0, ANY), (z0, ANY), (x0, ANY), mk, lnp, wp, wg, lnq, wo],
                               [(row_t, ANY), (row_t, ANY), (t_row, ANY), (ab_t, ANY)],
                               [ab_v, row_v, row_v, t_c, t_rows, vm((rows, c, cols), BF16), ab_rows, vm((RB, 2 * c, KB), F32), wpt_v, m_v, gq_v, dma((1, cl)), dma((2,)), dma((3,)), sq, sq, sq, sq, dma], 'mid')
        z2, dg1, dt1, gwo1, glq1 = call(turn_kernel, 3, [(ab1, ANY), (z1, ANY), (x1, ANY), (g, ANY), wg, lnq, wo],
                                        [(row_t, ANY), (row_t, ANY), (dt_t, ANY), f32_out(c, c), f32_out(2, c, 128)],
                                        [ab_v, row_v, row_v, row_v, row_v, t_c, t_rows, vm((RB, c, KB), BF16), t_rows, vm((RB, c, KB), F32), gq_v, dma((1, cl)), dma((3,)), dma((2,)), sq, sq, sq, sq, dma], 'turn')
        dmid, dg0, dt0, gwp1, gwg1, glp1, gwo0, glq0 = call(
            back_kernel, 4, [(ab1, ANY), (dt1, ANY), (z1, ANY), (x1, ANY), (dg1, ANY), (g, ANY), (t0, ANY), (x0, ANY), mk, lnp, wp, wg, lnq, wo],
            [(row_t, ANY), (row_t, ANY), (dt_t, ANY), f32_out(4 * c, c), f32_out(c, c), f32_out(2, 8, c), f32_out(c, c), f32_out(2, c, 128)],
            [ab_v, t_c, row_v, row_v, row_v, row_v, vm((rows, c, cols), BF16), row_v, ab_rows, vm((RB, 2 * c, KB), BF16), t_rows, vm((RB, c, KB), F32), wpt_v, m_v, gq_v, dma((2, cl)), dma((6,)), dma((2,)), sq, sq, sq, sq, dma], 'back')
        we, wc = 4 * c // n, c // n
        er, lr, gr = we + 3 * wc + 8, we + wc + 8, 2 * we + 4 * wc
        dz, grads, small = call(
            last_kernel, 5,
            [(ab0, ANY), (dt0, ANY), (z0, ANY), (x0, ANY), (dg0, ANY), (dmid, ANY), mk, lnp, wp, wg] + [(v, VM) for v in (gwp1, gwg1, gwo1, gwo0, glp1, glq1, glq0)],
            [(row_t, ANY), (jax.ShapeDtypeStruct((n, gr, c), BF16), ANY), f32_out(16, c)],
            [ab_v, t_c, row_v, row_v, row_v, row_v, ab_rows, vm((RB, 2 * c, KB_EDGE), BF16), wpt_v, m_v, vm((4 * c, c), F32), vm((c, c), F32), vm((2, 8, c), F32)]
            + [vm((n, k, c), F32) for k in (er, er, lr, lr)] + [vm((gr, c), BF16), dma((2, cl)), dma((4,)), dma, se, se, dma((3,)), dma((3,)), dma], 'last')

        def rows_of(start, count):
            return grads[:, start:start + count].reshape(n * count, c)

        base = 2 * we
        d_wp = jnp.stack([rows_of(we, we).T, rows_of(0, we).T])
        d_wg = jnp.stack([rows_of(base + 3 * wc, wc), rows_of(base, wc)])
        d_wo = jnp.stack([rows_of(base + 2 * wc, wc), rows_of(base + wc, wc)])
        small = small.astype(BF16)
        d_lp = jnp.stack([small[8:10], small[0:2]])
        d_lq = jnp.stack([small[4:6], small[2:4]])
        return z2, dz, d_lp, d_wp, d_wg, d_lq, d_wo

    full = P()
    return jax.shard_map(device_step, mesh=mesh, in_specs=(row_spec, mask_spec, row_spec, full, full, full, full, full), out_specs=(row_spec, row_spec, grad_spec, grad_spec, grad_spec, grad_spec, grad_spec), check_vma=False)
```

```python
import functools

import jax
import jax.numpy as jnp
from jax import lax
from jax.experimental import pallas as pl
from jax.experimental.pallas import tpu as pltpu
from jax.sharding import PartitionSpec as P

LN_EPS = 1e-5
AXIS = 'dap'
F32 = jnp.float32
BF16 = jnp.bfloat16
RB = 16
KB = 128
UNROLL = 2
MESH_ID = pl.DeviceIdType.MESH
ANY = pl.BlockSpec(memory_space=pl.ANY)
VM = pl.BlockSpec(memory_space=pltpu.VMEM)


def dot(lhs, rhs, lc, rc):
    return lax.dot_general(lhs, rhs, (((lc,), (rc,)), ((), ())), preferred_element_type=F32)


def norm(values, axis):
    mean = jnp.mean(values, axis=axis, keepdims=True)
    cent = values - mean
    var = jnp.mean(cent * cent, axis=axis, keepdims=True)
    rstd = lax.rsqrt(var + LN_EPS)
    return cent * rstd, rstd


def greet(n):
    me = lax.axis_index(AXIS)
    bar = pltpu.get_barrier_semaphore()

    def one(s, carry):
        pl.semaphore_signal(bar, inc=1, device_id={AXIS: lax.rem(me + s, n)}, device_id_type=MESH_ID)
        return carry

    lax.fori_loop(1, n, one, 0)
    return me


def meet(n):
    pl.semaphore_wait(pltpu.get_barrier_semaphore(), n - 1)


def scatter(n, me, src, dst, ssem, rsem):
    def one(s, carry):
        far = (s + 1) // 2
        peer = lax.rem(me + far * lax.rem(s, 2) + (n - far) * (1 - lax.rem(s, 2)), n)
        pltpu.make_async_remote_copy(src_ref=src(peer), dst_ref=dst(me), send_sem=ssem, recv_sem=rsem, device_id={AXIS: peer}, device_id_type=MESH_ID).start()
        return carry

    lax.fori_loop(1, n, one, 0)


def drain(ref, sem):
    pltpu.make_async_copy(ref, ref, sem).wait()


def drain_all(nq, part, sem):
    def one(q, carry):
        drain(part, sem(q))
        return carry

    lax.fori_loop(0, nq, one, 0)


def block(q, cols):
    per = cols // KB
    i0 = pl.multiple_of((q // per) * RB, RB)
    k0 = pl.multiple_of(lax.rem(q, per) * KB, KB)
    return pl.ds(i0, RB), pl.ds(k0, KB), i0


def pair_params(u, lnp_ref):
    return lnp_ref[u, 0:1, :].astype(F32), lnp_ref[u, 1:2, :].astype(F32)


def load_wpt(u, wp_ref, wpt_v):
    wpt_v[u] = wp_ref[u].astype(F32).T.astype(BF16)


def load_mask(m_ref, m_v):
    for r in range(m_v.shape[0]):
        m_v[r, 0:1, :] = m_ref[r:r + 1, :].astype(F32)


def load_chan(u, lnq_ref, gq_v):
    c = gq_v.shape[2]
    for h in range(2):
        row = lnq_ref[u, h:h + 1, :].astype(F32)
        col = jnp.broadcast_to(row, (128, c)).T
        for l in range(gq_v.shape[3] // 128):
            gq_v[u, h, :, l * 128:(l + 1) * 128] = col


def pack(s_ref, e0, count, write):
    def one(e, carry):
        off = pl.multiple_of(e * 8, 8)
        val = s_ref[:, pl.ds(e0 + off, 8), :]
        write(pl.ds(off, 8), jnp.swapaxes(val, 0, 1).astype(BF16))
        return carry

    lax.fori_loop(0, count // 8, one, 0)


def unpack(read, count, write):
    def one(e, carry):
        sl = pl.ds(pl.multiple_of(e * 16, 16), 16)
        write(sl, jnp.swapaxes(read(sl).astype(F32), 0, 1).astype(BF16))
        return carry

    lax.fori_loop(0, count // 16, one, 0)


def each_row(row):
    lax.fori_loop(0, RB, row, 0, unroll=UNROLL)


def project(s_ref, i, x_row, m_row, w_t, c):
    p = dot(w_t, x_row, 1, 1)
    s_ref[i, 0:c, :] = m_row * jax.nn.sigmoid(p[c:2 * c]) * p[0:c]
    s_ref[i, c:2 * c, :] = m_row * jax.nn.sigmoid(p[3 * c:]) * p[2 * c:3 * c]


def fold_rows(v):
    return jnp.sum(v.reshape(v.shape[0] // 8, 8, v.shape[1]), axis=0)


def fold_lanes(v):
    out = v[:, 0:128]
    for h in range(1, v.shape[1] // 128):
        out = out + v[:, h * 128:(h + 1) * 128]
    return out


def pack_ab(s_ref, c, abr, ri, rk):
    for h in range(2):
        def write(sl, val, h=h):
            abr[h, sl, ri, rk] = val
        pack(s_ref, h * c, c, write)


def unpack_dab(abr, dab_t, c, ri, rk):
    for h in range(2):
        def write_t(sl, val, h=h):
            dab_t[:, pl.ds(pl.multiple_of(h * c + sl.start, 16), 16), :] = val
        unpack(lambda sl, h=h: abr[h, sl, ri, rk], c, write_t)


def finish_back(i, r, rk, dn, th, rstd, y, upd, gate, gain, w_out, dg_v, s_ref, gwo, glq, u):
    d_gate = dn * upd * gate * (1.0 - gate)
    d_upd = (dn * gate).astype(BF16)
    dg_v[r, rk, :] = d_gate.astype(BF16)
    gwo[u] += dot(y, d_upd, 1, 0)
    dy = dot(w_out, d_upd, 1, 1).astype(BF16).astype(F32)
    glq[u, 0] += fold_lanes(dy * th)
    glq[u, 1] += fold_lanes(dy)
    dyg = dy * gain
    m1 = jnp.mean(dyg, axis=0, keepdims=True)
    m2 = jnp.mean(dyg * th, axis=0, keepdims=True)
    s_ref[i, 0:dy.shape[0], :] = rstd * (dyg - m1 - th * m2)


def project_back(u, i, r, rk, dab_t, m_v, x_v, z_v, dg_v, dn_v, gain, wpt_v, wp_ref, wg_ref, gwp, gwg, glp, c):
    x_row = x_v[r, rk, :]
    m_row = m_v[r, 0:1, rk]
    p = dot(wpt_v[u], x_row, 1, 1)
    parts = []
    for h in range(2):
        d_val = dab_t[i, h * c:(h + 1) * c, :].astype(F32) * m_row
        lin = p[2 * h * c:(2 * h + 1) * c]
        sig = jax.nn.sigmoid(p[(2 * h + 1) * c:(2 * h + 2) * c])
        d_lin = d_val * sig
        parts.append(d_lin.astype(BF16))
        parts.append((d_lin * lin * (1.0 - sig)).astype(BF16))
    d_proj = jnp.concatenate(parts, axis=0)
    d_gate = dg_v[r, rk, :]
    gwp[u] += dot(d_proj, x_row, 1, 0)
    gwg[u] += dot(x_row, d_gate, 0, 0)
    dxt = dot(wp_ref[u], d_proj, 1, 0) + dot(wg_ref[u], d_gate, 1, 1)
    dx = dxt.T.astype(BF16).astype(F32)
    xh, rstd = norm(z_v[r, rk, :].astype(F32), -1)
    glp[u, 0] += fold_rows(dx * xh)
    glp[u, 1] += fold_rows(dx)
    dxg = dx * gain
    m1 = jnp.mean(dxg, axis=-1, keepdims=True)
    m2 = jnp.mean(dxg * xh, axis=-1, keepdims=True)
    return (dn_v[r, rk, :].astype(F32) + rstd * (dxg - m1 - xh * m2)).astype(BF16)


def to_pair(n, me, src, dst, ssem, rsem):
    partner = me + 1 - 2 * lax.rem(me, 2)
    pltpu.make_async_remote_copy(src_ref=src, dst_ref=dst, send_sem=ssem, recv_sem=rsem, device_id={AXIS: partner}, device_id_type=MESH_ID).start()


def to_chips(n, me, src, dst, ssem, rsem):
    core, chip = lax.rem(me, 2), me // 2

    def one(s, carry):
        other = lax.rem(chip + s, n // 2)
        pltpu.make_async_remote_copy(src_ref=src(other), dst_ref=dst(chip), send_sem=ssem, recv_sem=rsem, device_id={AXIS: 2 * other + core}, device_id_type=MESH_ID).start()
        return carry

    lax.fori_loop(1, n // 2, one, 0)


def pair_sum(core, parts, pair_in, comb):
    def one(z, carry):
        comb[z] = parts[z, core] + pair_in[z]
        return carry

    lax.fori_loop(0, comb.shape[0], one, 0)


def add_parts(recv):
    def one(s, acc):
        return acc + recv[s]

    return lax.fori_loop(1, recv.shape[0], one, recv[0])


def whole_kernel(n, z_hbm, m_ref, g_hbm, lnp_ref, wp_ref, wg_ref, lnq_ref, wo_ref,
                 zo_hbm, dz_hbm, x0_hbm, t0_hbm, grads_ref, small_ref,
                 ab0, ab1, abr, ts, tr, dt, z_v, x_v, g_v, dg_v, s_ref, dab_t, t_c, xp_c, zo_c,
                 wpt_v, gq_v, m_v, gwp, gwg, gwo, glp, glq,
                 early, pair_e, comb_e, gath_e, late, pair_l, comb_l, gath_l, mine, all_v,
                 sems, isem, osem, gss, grs):
    rows, cols, c = z_v.shape
    cl = c // n
    nq = (rows // RB) * (cols // KB)
    we, wc = 4 * c // n, c // n
    load_z = pltpu.make_async_copy(z_hbm, z_v, isem.at[0])
    load_g = pltpu.make_async_copy(g_hbm, g_v, isem.at[1])
    load_z.start()
    load_g.start()
    me = greet(n)
    core, chip = lax.rem(me, 2), me // 2

    def snd(k):
        return lambda q: sems.at[k, 0, q]

    def rcv(k):
        return lambda q: sems.at[k, 1, q]

    ab_part = ab0.at[:, :, pl.ds(0, RB * (n - 1)), pl.ds(0, KB)]
    dt_part = dt.at[:, pl.ds(0, RB * (n - 1)), pl.ds(0, KB)]
    t_part = tr.at[pl.ds(0, c - cl), pl.ds(0, RB), pl.ds(0, KB)]
    dab_part = abr.at[:, pl.ds(0, c - cl), pl.ds(0, RB), pl.ds(0, KB)]

    def send_ab(k, q, dest):
        ri, rk, i0 = block(q, cols)

        def at(dev):
            return pl.ds(pl.multiple_of(dev * rows + i0, RB), RB)

        scatter(n, me, lambda p: abr.at[:, pl.ds(p * cl, cl), ri, rk], lambda d: dest.at[:, :, at(d), rk], snd(k)(q), rcv(k)(q))

        def own(j, carry):
            for h in range(2):
                dest[h, j, at(me), rk] = abr[h, me * cl + j, ri, rk]
            return carry

        lax.fori_loop(0, cl, own, 0)

    def send_dt(k, q):
        ri, rk, i0 = block(q, cols)

        def at(dev):
            return pl.ds(pl.multiple_of(dev * rows + i0, RB), RB)

        scatter(n, me, lambda p: tr.at[pl.ds(p * cl, cl), ri, rk], lambda d: dt.at[:, at(d), rk], snd(k)(q), rcv(k)(q))

        def own(j, carry):
            dt[j, at(me), rk] = tr[me * cl + j, ri, rk]
            return carry

        lax.fori_loop(0, cl, own, 0)

    def exchange(product, send):
        def one(j, carry):
            product(j)
            send(j, 1, 0)
            return carry

        lax.fori_loop(0, cl, one, 0)

        def rest(q, carry):
            send(0, cl, q)
            return carry

        lax.fori_loop(1, nq, rest, 0)

    def exchange_t(k, product):
        def send(j, count, q):
            ri, rk, i0 = block(q, cols)
            scatter(n, me, lambda p: ts.at[pl.ds(j, count), pl.ds(pl.multiple_of(p * rows + i0, RB), RB), rk], lambda d: tr.at[pl.ds(d * cl + j, count), ri, rk], snd(k)(q), rcv(k)(q))

        exchange(product, send)

        def own(j, carry):
            tr[me * cl + j, :, :] = ts[j, pl.ds(pl.multiple_of(me * rows, RB), rows), :]
            return carry

        lax.fori_loop(0, cl, own, 0)

    def exchange_dab(k, incoming, ab):
        def product(j):
            left, right, d_t = ab[0, j], ab[1, j], dt[j]
            if incoming:
                d_left = dot(right, d_t, 1, 1)
                d_right = dot(left, d_t, 1, 0)
            else:
                d_left = dot(d_t, right, 1, 0)
                d_right = dot(d_t, left, 0, 0)
            ab[0, j, :, :] = d_left.astype(BF16)
            ab[1, j, :, :] = d_right.astype(BF16)

        def send(j, count, q):
            ri, rk, i0 = block(q, cols)
            scatter(n, me, lambda p: ab.at[:, pl.ds(j, count), pl.ds(pl.multiple_of(p * rows + i0, RB), RB), rk], lambda d: abr.at[:, pl.ds(d * cl + j, count), ri, rk], snd(k)(q), rcv(k)(q))

        exchange(product, send)

        def own(j, carry):
            for h in range(2):
                abr[h, me * cl + j, :, :] = ab[h, j, pl.ds(pl.multiple_of(me * rows, RB), rows), :]
            return carry

        lax.fori_loop(0, cl, own, 0)

    load_wpt(0, wp_ref, wpt_v)
    load_mask(m_ref, m_v)
    gain0, shift0 = pair_params(0, lnp_ref)
    gain1, shift1 = pair_params(1, lnp_ref)
    load_z.wait()

    def step1(q, carry):
        ri, rk, i0 = block(q, cols)

        def row(i, carry2):
            r = i0 + i
            xh, _ = norm(z_v[r, rk, :].astype(F32), -1)
            x_row = (xh * gain0 + shift0).astype(BF16)
            x_v[r, rk, :] = x_row
            project(s_ref, i, x_row, m_v[r, 0:1, rk], wpt_v[0], c)
            return carry2

        each_row(row)
        pack_ab(s_ref, c, abr, ri, rk)

        @pl.when(q == 0)
        def _():
            meet(n)

        send_ab(0, q, ab0)
        pltpu.make_async_copy(x_v.at[ri, rk, :], x0_hbm.at[ri, rk, :], osem.at[0]).start()
        return carry

    lax.fori_loop(0, nq, step1, 0)
    load_wpt(1, wp_ref, wpt_v)
    for u in range(2):
        load_chan(u, lnq_ref, gq_v)
    for ref in (gwp, gwg, gwo, glp, glq):
        ref[...] = jnp.zeros_like(ref)
    drain(x_v, osem.at[0])
    drain_all(nq, ab_part, snd(0))
    drain_all(nq, ab_part, rcv(0))

    def product0(j):
        ts[j, :, :] = dot(ab0[0, j], ab0[1, j], 1, 1).astype(BF16)

    exchange_t(1, product0)

    def step2(q, carry):
        ri, rk, i0 = block(q, cols)

        @pl.when(q > 0)
        def _():
            drain(t_c, osem.at[1])

        drain(t_part, rcv(1)(q))

        def write_t(sl, val):
            t_c[:, sl, :] = val

        unpack(lambda sl: tr[sl, ri, rk], c, write_t)
        pltpu.make_async_copy(t_c, t0_hbm.at[ri, :, rk], osem.at[1]).start()

        def row(i, carry2):
            r = i0 + i
            th, _ = norm(t_c[i].astype(F32), 0)
            y = (th * gq_v[0, 0] + gq_v[0, 1]).astype(BF16)
            upd = dot(y, wo_ref[0], 0, 0)
            gate = jax.nn.sigmoid(dot(x_v[r, rk, :], wg_ref[0], 1, 0))
            z_new = (z_v[r, rk, :].astype(F32) + gate * upd).astype(BF16)
            z_v[r, rk, :] = z_new
            xh, _ = norm(z_new.astype(F32), -1)
            x_row = (xh * gain1 + shift1).astype(BF16)
            x_v[r, rk, :] = x_row
            project(s_ref, i, x_row, m_v[r, 0:1, rk], wpt_v[1], c)
            return carry2

        each_row(row)
        pack_ab(s_ref, c, abr, ri, rk)
        send_ab(2, q, ab1)
        return carry

    lax.fori_loop(0, nq, step2, 0)
    drain(t_c, osem.at[1])
    drain_all(nq, t_part, snd(1))
    drain_all(nq, ab_part, snd(2))
    load_g.wait()
    drain_all(nq, ab_part, rcv(2))

    def product1(j):
        ts[j, :, :] = dot(ab1[0, j], ab1[1, j], 0, 0).astype(BF16)

    exchange_t(3, product1)

    def step3(q, carry):
        ri, rk, i0 = block(q, cols)
        drain(t_part, rcv(3)(q))

        def write_t(sl, val):
            t_c[:, sl, :] = val

        unpack(lambda sl: tr[sl, ri, rk], c, write_t)

        @pl.when(q > 0)
        def _():
            drain(zo_c, osem.at[2])

        def row(i, carry2):
            r = i0 + i
            th, rstd = norm(t_c[i].astype(F32), 0)
            y = (th * gq_v[1, 0] + gq_v[1, 1]).astype(BF16)
            upd = dot(y, wo_ref[1], 0, 0)
            gate = jax.nn.sigmoid(dot(x_v[r, rk, :], wg_ref[1], 1, 0))
            zo_c[i] = (z_v[r, rk, :].astype(F32) + gate * upd).astype(BF16)
            finish_back(i, r, rk, g_v[r, rk, :].astype(F32), th, rstd, y, upd, gate, gq_v[1, 0], wo_ref[1], dg_v, s_ref, gwo, glq, 1)
            return carry2

        each_row(row)
        pltpu.make_async_copy(zo_c, zo_hbm.at[ri, rk, :], osem.at[2]).start()

        def write(sl, val):
            tr[sl, ri, rk] = val

        pack(s_ref, 0, c, write)
        send_dt(4, q)
        return carry

    lax.fori_loop(0, nq, step3, 0)
    drain(zo_c, osem.at[2])
    drain_all(nq, t_part, snd(3))
    drain_all(nq, dt_part, snd(4))
    drain_all(nq, dt_part, rcv(4))
    exchange_dab(5, True, ab1)

    def step4(q, carry):
        ri, rk, i0 = block(q, cols)
        load_t = pltpu.make_async_copy(t0_hbm.at[ri, :, rk], t_c, isem.at[2])
        load_x = pltpu.make_async_copy(x0_hbm.at[ri, rk, :], xp_c, isem.at[3])
        load_t.start()
        load_x.start()
        drain(dab_part, rcv(5)(q))
        unpack_dab(abr, dab_t, c, ri, rk)
        load_t.wait()
        load_x.wait()

        def row(i, carry2):
            r = i0 + i
            dn = project_back(1, i, r, rk, dab_t, m_v, x_v, z_v, dg_v, g_v, gain1, wpt_v, wp_ref, wg_ref, gwp, gwg, glp, c)
            g_v[r, rk, :] = dn
            th, rstd = norm(t_c[i].astype(F32), 0)
            y = (th * gq_v[0, 0] + gq_v[0, 1]).astype(BF16)
            upd = dot(y, wo_ref[0], 0, 0)
            gate = jax.nn.sigmoid(dot(xp_c[i], wg_ref[0], 1, 0))
            finish_back(i, r, rk, dn.astype(F32), th, rstd, y, upd, gate, gq_v[0, 0], wo_ref[0], dg_v, s_ref, gwo, glq, 0)
            return carry2

        each_row(row)

        def write(sl, val):
            tr[sl, ri, rk] = val

        pack(s_ref, 0, c, write)
        send_dt(6, q)
        return carry

    lax.fori_loop(0, nq, step4, 0)
    reload_z = pltpu.make_async_copy(z_hbm, z_v, isem.at[0])
    reload_x = pltpu.make_async_copy(x0_hbm, x_v, isem.at[1])
    reload_z.start()
    reload_x.start()
    small = [jnp.sum(glp[1, h], axis=0, keepdims=True) for h in range(2)]
    small += [jnp.sum(glq[u, h].T, axis=0, keepdims=True) for u in (1, 0) for h in range(2)]
    small = jnp.concatenate(small + [jnp.zeros((2, c), F32)], axis=0)
    e1, e2, e3, e4 = we, we + wc, we + 2 * wc, we + 3 * wc

    def fill(p, carry):
        z, k = p // 2, lax.rem(p, 2)
        cut = pl.ds(pl.multiple_of(p * wc, 8), wc)
        early[z, k, 0:e1, :] = gwp[1, pl.ds(pl.multiple_of(p * we, 8), we), :]
        early[z, k, e1:e2, :] = gwg[1, cut, :]
        early[z, k, e2:e3, :] = gwo[1, cut, :]
        early[z, k, e3:e4, :] = gwo[0, cut, :]
        early[z, k, e4:e4 + 8, :] = small
        return carry

    lax.fori_loop(0, n, fill, 0)
    to_pair(n, me, early.at[:, 1 - core], pair_e, gss.at[0], grs.at[0])
    drain_all(nq, dab_part, snd(5))
    drain_all(nq, dt_part, snd(6))
    drain_all(nq, dt_part, rcv(6))
    exchange_dab(7, False, ab0)
    drain(pair_e, grs.at[0])
    pair_sum(core, early, pair_e, comb_e)
    gath_e[chip] = comb_e[chip]
    to_chips(n, me, lambda o: comb_e.at[o], lambda d: gath_e.at[d], gss.at[1], grs.at[1])
    reload_z.wait()
    reload_x.wait()

    def step5(q, carry):
        ri, rk, i0 = block(q, cols)
        drain(dab_part, rcv(7)(q))
        unpack_dab(abr, dab_t, c, ri, rk)

        def row(i, carry2):
            r = i0 + i
            g_v[r, rk, :] = project_back(0, i, r, rk, dab_t, m_v, x_v, z_v, dg_v, g_v, gain0, wpt_v, wp_ref, wg_ref, gwp, gwg, glp, c)
            return carry2

        each_row(row)
        pltpu.make_async_copy(g_v.at[ri, rk, :], dz_hbm.at[ri, rk, :], osem.at[3]).start()
        return carry

    lax.fori_loop(0, nq, step5, 0)
    tail = jnp.concatenate([jnp.sum(glp[0, h], axis=0, keepdims=True) for h in range(2)] + [jnp.zeros((6, c), F32)], axis=0)

    def fill_late(p, carry):
        z, k = p // 2, lax.rem(p, 2)
        late[z, k, 0:e1, :] = gwp[0, pl.ds(pl.multiple_of(p * we, 8), we), :]
        late[z, k, e1:e2, :] = gwg[0, pl.ds(pl.multiple_of(p * wc, 8), wc), :]
        late[z, k, e2:e2 + 8, :] = tail
        return carry

    lax.fori_loop(0, n, fill_late, 0)
    to_pair(n, me, late.at[:, 1 - core], pair_l, gss.at[2], grs.at[2])
    drain(gath_e.at[pl.ds(0, n // 2 - 1)], grs.at[1])
    sum_e = add_parts(gath_e)
    drain(pair_l, grs.at[2])
    pair_sum(core, late, pair_l, comb_l)
    gath_l[chip] = comb_l[chip]
    to_chips(n, me, lambda o: comb_l.at[o], lambda d: gath_l.at[d], gss.at[3], grs.at[3])
    drain(gath_l.at[pl.ds(0, n // 2 - 1)], grs.at[3])
    sum_l = add_parts(gath_l)
    mine[...] = jnp.concatenate([sum_e[0:e1], sum_l[0:e1], sum_e[e1:e4], sum_l[e1:e2]], axis=0).astype(BF16)
    to_chips(n, me, lambda o: mine, lambda d: all_v.at[core, d], gss.at[4], grs.at[4])
    all_v[core, chip] = mine[...]
    small_ref[0:8, :] = sum_e[e4:e4 + 8]
    small_ref[8:16, :] = sum_l[e2:e2 + 8]
    drain(dz_hbm, osem.at[3])
    drain_all(nq, dab_part, snd(7))
    drain(pair_e, gss.at[0])
    drain(gath_e.at[pl.ds(0, n // 2 - 1)], gss.at[1])
    drain(pair_l, gss.at[2])
    drain(gath_l.at[pl.ds(0, n // 2 - 1)], gss.at[3])
    others = all_v.at[0, pl.ds(0, n // 2 - 1)]
    drain(others, gss.at[4])
    drain(others, grs.at[4])
    to_pair(n, me, all_v.at[core], all_v.at[core], gss.at[5], grs.at[5])
    drain(all_v.at[core], gss.at[5])
    drain(all_v.at[1 - core], grs.at[5])
    grads_ref[...] = all_v[...]


def solution(mesh):
    row_spec = P(('data', AXIS), None, None)
    mask_spec = P(('data', AXIS), None)
    grad_spec = P('data', None, None)
    n = mesh.shape[AXIS]

    def device_step(z0, mask, g, ln_pair, w_proj, w_gate, ln_chan, w_out):
        rows, cols, c = z0.shape
        cl = c // n
        nq = (rows // RB) * (cols // KB)
        we, wc = 4 * c // n, c // n
        er, lr, gr = we + 3 * wc + 8, we + wc + 8, 2 * we + 4 * wc
        half = n // 2
        vm = pltpu.VMEM
        dma = pltpu.SemaphoreType.DMA
        row_t = jax.ShapeDtypeStruct((rows, cols, c), BF16)
        row_v = vm((rows, cols, c), BF16)
        chan_v = vm((cl, cols, cols), BF16)
        scratch = [vm((2, cl, cols, cols), BF16)] * 2 + [vm((2, c, rows, cols), BF16), chan_v, vm((c, rows, cols), BF16), chan_v] + [row_v] * 4
        scratch += [vm((RB, 2 * c, KB), F32), vm((RB, 2 * c, KB), BF16), vm((RB, c, KB), BF16), vm((RB, KB, c), BF16), vm((RB, KB, c), BF16)]
        scratch += [vm((2, 4 * c, c), BF16), vm((2, 2, c, KB), F32), vm((rows, 1, cols), F32)]
        scratch += [vm((2, 4 * c, c), F32), vm((2, c, c), F32), vm((2, c, c), F32), vm((2, 2, 8, c), F32), vm((2, 2, c, 128), F32)]
        for k in (er, lr):
            scratch += [vm((half, 2, k, c), F32)] + [vm((half, k, c), F32)] * 3
        scratch += [vm((gr, c), BF16), vm((2, half, gr, c), BF16)]
        scratch += [dma((8, 2, nq)), dma((4,)), dma((4,)), dma((6,)), dma((6,))]
        z2, dz, _, _, grads, small = pl.pallas_call(
            functools.partial(whole_kernel, n),
            out_shape=(row_t, row_t, row_t, jax.ShapeDtypeStruct((rows, c, cols), BF16), jax.ShapeDtypeStruct((2, half, gr, c), BF16), jax.ShapeDtypeStruct((16, c), F32)),
            in_specs=[ANY, VM, ANY] + [VM] * 5,
            out_specs=(ANY, ANY, ANY, ANY, VM, VM),
            scratch_shapes=scratch,
            compiler_params=pltpu.CompilerParams(collective_id=1, has_side_effects=True, vmem_limit_bytes=67043328),
            name='whole',
        )(z0, mask, g, ln_pair, w_proj, w_gate, ln_chan, w_out)

        def rows_of(start, count):
            return jnp.swapaxes(grads[:, :, start:start + count], 0, 1).reshape(n * count, c)

        base = 2 * we
        d_wp = jnp.stack([rows_of(we, we).T, rows_of(0, we).T])
        d_wg = jnp.stack([rows_of(base + 3 * wc, wc), rows_of(base, wc)])
        d_wo = jnp.stack([rows_of(base + 2 * wc, wc), rows_of(base + wc, wc)])
        small = small.astype(BF16)
        d_lp = jnp.stack([small[8:10], small[0:2]])
        d_lq = jnp.stack([small[4:6], small[2:4]])
        return z2, dz, d_lp, d_wp, d_wg, d_lq, d_wo

    full = P()
    return jax.shard_map(device_step, mesh=mesh, in_specs=(row_spec, mask_spec, row_spec, full, full, full, full, full), out_specs=(row_spec, row_spec, grad_spec, grad_spec, grad_spec, grad_spec, grad_spec), check_vma=False)
```

```python
import functools

import jax
import jax.numpy as jnp
from jax import lax
from jax.experimental import pallas as pl
from jax.experimental.pallas import tpu as pltpu
from jax.sharding import PartitionSpec as P

LN_EPS = 1e-5
AXIS = 'dap'
F32 = jnp.float32
BF16 = jnp.bfloat16
RB = 16
KB = 128
UNROLL = 2
MESH_ID = pl.DeviceIdType.MESH
ANY = pl.BlockSpec(memory_space=pl.ANY)
VM = pl.BlockSpec(memory_space=pltpu.VMEM)


def dot(lhs, rhs, lc, rc):
    return lax.dot_general(lhs, rhs, (((lc,), (rc,)), ((), ())), preferred_element_type=F32)


def norm(values, axis):
    mean = jnp.mean(values, axis=axis, keepdims=True)
    cent = values - mean
    var = jnp.mean(cent * cent, axis=axis, keepdims=True)
    rstd = lax.rsqrt(var + LN_EPS)
    return cent * rstd, rstd


def greet(n):
    me = lax.axis_index(AXIS)
    bar = pltpu.get_barrier_semaphore()

    def one(s, carry):
        pl.semaphore_signal(bar, inc=1, device_id={AXIS: lax.rem(me + s, n)}, device_id_type=MESH_ID)
        return carry

    lax.fori_loop(1, n, one, 0)
    return me


def meet(n):
    pl.semaphore_wait(pltpu.get_barrier_semaphore(), n - 1)


def scatter(n, me, src, dst, ssem, rsem):
    def one(s, carry):
        far = (s + 1) // 2
        peer = lax.rem(me + far * lax.rem(s, 2) + (n - far) * (1 - lax.rem(s, 2)), n)
        pltpu.make_async_remote_copy(src_ref=src(peer), dst_ref=dst(me), send_sem=ssem, recv_sem=rsem, device_id={AXIS: peer}, device_id_type=MESH_ID).start()
        return carry

    lax.fori_loop(1, n, one, 0)


def drain(ref, sem):
    pltpu.make_async_copy(ref, ref, sem).wait()


def drain_all(nq, part, sem):
    def one(q, carry):
        drain(part, sem(q))
        return carry

    lax.fori_loop(0, nq, one, 0)


def block(q, cols):
    per = cols // KB
    i0 = pl.multiple_of((q // per) * RB, RB)
    k0 = pl.multiple_of(lax.rem(q, per) * KB, KB)
    return pl.ds(i0, RB), pl.ds(k0, KB), i0


def pair_params(u, lnp_ref):
    return lnp_ref[u, 0:1, :].astype(F32), lnp_ref[u, 1:2, :].astype(F32)


def load_wpt(u, wp_ref, wpt_v):
    wpt_v[u] = wp_ref[u].astype(F32).T.astype(BF16)


def load_mask(m_ref, m_v):
    for r in range(m_v.shape[0]):
        m_v[r, 0:1, :] = m_ref[r:r + 1, :].astype(F32)


def load_chan(u, lnq_ref, gq_v):
    c = gq_v.shape[2]
    for h in range(2):
        row = lnq_ref[u, h:h + 1, :].astype(F32)
        col = jnp.broadcast_to(row, (128, c)).T
        for l in range(gq_v.shape[3] // 128):
            gq_v[u, h, :, l * 128:(l + 1) * 128] = col


def pack(s_ref, e0, count, write):
    def one(e, carry):
        off = pl.multiple_of(e * 8, 8)
        val = s_ref[:, pl.ds(e0 + off, 8), :]
        write(pl.ds(off, 8), jnp.swapaxes(val, 0, 1).astype(BF16))
        return carry

    lax.fori_loop(0, count // 8, one, 0)


def unpack(read, count, write):
    def one(e, carry):
        sl = pl.ds(pl.multiple_of(e * 16, 16), 16)
        write(sl, jnp.swapaxes(read(sl).astype(F32), 0, 1).astype(BF16))
        return carry

    lax.fori_loop(0, count // 16, one, 0)


def each_row(row):
    def pair(k, carry):
        return row(2 * k, carry)

    lax.fori_loop(0, RB // 2, pair, 0, unroll=UNROLL)


def get_rows(ref, r, rk):
    return ref[pl.ds(r, 2), rk, :].reshape(2 * KB, ref.shape[2])


def put_rows(ref, r, rk, val):
    ref[pl.ds(r, 2), rk, :] = val.reshape(2, KB, val.shape[1])


def get_lanes(ref, i, lo, hi):
    return jnp.concatenate([ref[i, lo:hi, :].astype(F32), ref[i + 1, lo:hi, :].astype(F32)], axis=1)


def put_lanes(ref, i, lo, hi, val):
    ref[i, lo:hi, :] = val[:, :KB]
    ref[i + 1, lo:hi, :] = val[:, KB:]


def get_mask(m_v, r, rk):
    return jnp.concatenate([m_v[r, 0:1, rk], m_v[r + 1, 0:1, rk]], axis=1)


def project(s_ref, i, x_row, m_row, w_t, c):
    p = dot(w_t, x_row, 1, 1)
    put_lanes(s_ref, i, 0, c, m_row * jax.nn.sigmoid(p[c:2 * c]) * p[0:c])
    put_lanes(s_ref, i, c, 2 * c, m_row * jax.nn.sigmoid(p[3 * c:]) * p[2 * c:3 * c])


def fold_rows(v):
    return jnp.sum(v.reshape(v.shape[0] // 8, 8, v.shape[1]), axis=0)


def fold_lanes(v):
    out = v[:, 0:128]
    for h in range(1, v.shape[1] // 128):
        out = out + v[:, h * 128:(h + 1) * 128]
    return out


def pack_ab(s_ref, c, abr, ri, rk):
    for h in range(2):
        def write(sl, val, h=h):
            abr[h, sl, ri, rk] = val
        pack(s_ref, h * c, c, write)


def unpack_dab(abr, dab_t, c, ri, rk):
    for h in range(2):
        def write_t(sl, val, h=h):
            dab_t[:, pl.ds(pl.multiple_of(h * c + sl.start, 16), 16), :] = val
        unpack(lambda sl, h=h: abr[h, sl, ri, rk], c, write_t)


def finish_back(i, r, rk, dn, th, rstd, y, upd, gate, gain, w_out, dg_v, s_ref, gwo, glq, u):
    d_gate = dn * upd * gate * (1.0 - gate)
    d_upd = (dn * gate).astype(BF16)
    put_rows(dg_v, r, rk, d_gate.astype(BF16))
    gwo[u] += dot(y, d_upd, 1, 0)
    dy = dot(w_out, d_upd, 1, 1).astype(BF16).astype(F32)
    glq[u, 0] += fold_lanes(dy * th)
    glq[u, 1] += fold_lanes(dy)
    dyg = dy * gain
    m1 = jnp.mean(dyg, axis=0, keepdims=True)
    m2 = jnp.mean(dyg * th, axis=0, keepdims=True)
    put_lanes(s_ref, i, 0, dy.shape[0], rstd * (dyg - m1 - th * m2))


def project_back(u, i, r, rk, dab_t, m_v, x_v, z_v, dg_v, dn_v, gain, wpt_v, wp_ref, wg_ref, gwp, gwg, glp, c):
    x_row = get_rows(x_v, r, rk)
    m_row = get_mask(m_v, r, rk)
    p = dot(wpt_v[u], x_row, 1, 1)
    parts = []
    for h in range(2):
        d_val = get_lanes(dab_t, i, h * c, (h + 1) * c) * m_row
        lin = p[2 * h * c:(2 * h + 1) * c]
        sig = jax.nn.sigmoid(p[(2 * h + 1) * c:(2 * h + 2) * c])
        d_lin = d_val * sig
        parts.append(d_lin.astype(BF16))
        parts.append((d_lin * lin * (1.0 - sig)).astype(BF16))
    d_proj = jnp.concatenate(parts, axis=0)
    d_gate = get_rows(dg_v, r, rk)
    gwp[u] += dot(d_proj, x_row, 1, 0)
    gwg[u] += dot(x_row, d_gate, 0, 0)
    dxt = dot(wp_ref[u], d_proj, 1, 0) + dot(wg_ref[u], d_gate, 1, 1)
    dx = dxt.T.astype(BF16).astype(F32)
    xh, rstd = norm(get_rows(z_v, r, rk).astype(F32), -1)
    glp[u, 0] += fold_rows(dx * xh)
    glp[u, 1] += fold_rows(dx)
    dxg = dx * gain
    m1 = jnp.mean(dxg, axis=-1, keepdims=True)
    m2 = jnp.mean(dxg * xh, axis=-1, keepdims=True)
    return (get_rows(dn_v, r, rk).astype(F32) + rstd * (dxg - m1 - xh * m2)).astype(BF16)


def to_pair(n, me, src, dst, ssem, rsem):
    partner = me + 1 - 2 * lax.rem(me, 2)
    pltpu.make_async_remote_copy(src_ref=src, dst_ref=dst, send_sem=ssem, recv_sem=rsem, device_id={AXIS: partner}, device_id_type=MESH_ID).start()


def to_chips(n, me, src, dst, ssem, rsem):
    core, chip = lax.rem(me, 2), me // 2

    def one(s, carry):
        other = lax.rem(chip + s, n // 2)
        pltpu.make_async_remote_copy(src_ref=src(other), dst_ref=dst(chip), send_sem=ssem, recv_sem=rsem, device_id={AXIS: 2 * other + core}, device_id_type=MESH_ID).start()
        return carry

    lax.fori_loop(1, n // 2, one, 0)


def pair_sum(core, parts, pair_in, comb):
    def one(z, carry):
        comb[z] = parts[z, core] + pair_in[z]
        return carry

    lax.fori_loop(0, comb.shape[0], one, 0)


def add_parts(recv):
    def one(s, acc):
        return acc + recv[s]

    return lax.fori_loop(1, recv.shape[0], one, recv[0])


def whole_kernel(n, z_hbm, m_ref, g_hbm, lnp_ref, wp_ref, wg_ref, lnq_ref, wo_ref,
                 zo_hbm, dz_hbm, x0_hbm, t0_hbm, grads_ref, small_ref,
                 ab0, ab1, abr, ts, tr, dt, z_v, x_v, g_v, dg_v, s_ref, dab_t, t_c, xp_c, zo_c,
                 wpt_v, gq_v, m_v, gwp, gwg, gwo, glp, glq,
                 early, pair_e, comb_e, gath_e, late, pair_l, comb_l, gath_l, mine, all_v,
                 sems, isem, osem, gss, grs):
    rows, cols, c = z_v.shape
    cl = c // n
    nq = (rows // RB) * (cols // KB)
    we, wc = 4 * c // n, c // n
    load_z = pltpu.make_async_copy(z_hbm, z_v, isem.at[0])
    load_g = pltpu.make_async_copy(g_hbm, g_v, isem.at[1])
    load_z.start()
    load_g.start()
    me = greet(n)
    core, chip = lax.rem(me, 2), me // 2

    def snd(k, h=0):
        return lambda q: sems.at[k, h, 0, q]

    def rcv(k, h=0):
        return lambda q: sems.at[k, h, 1, q]

    hc = cl // 2

    ab_part = ab0.at[:, pl.ds(0, cl // 2), pl.ds(0, RB * (n - 1)), pl.ds(0, KB)]
    dt_part = dt.at[pl.ds(0, cl // 2), pl.ds(0, RB * (n - 1)), pl.ds(0, KB)]
    t_part = tr.at[pl.ds(0, c - cl), pl.ds(0, RB), pl.ds(0, KB)]
    dab_part = abr.at[:, pl.ds(0, c - cl), pl.ds(0, RB), pl.ds(0, KB)]

    def send_ab(k, q, dest):
        ri, rk, i0 = block(q, cols)

        def at(dev):
            return pl.ds(pl.multiple_of(dev * rows + i0, RB), RB)

        for e in range(2):
            scatter(n, me, lambda p, e=e: abr.at[:, pl.ds(p * cl + e * hc, hc), ri, rk], lambda d, e=e: dest.at[:, pl.ds(e * hc, hc), at(d), rk], snd(k, e)(q), rcv(k, e)(q))

        def own(j, carry):
            for h in range(2):
                dest[h, j, at(me), rk] = abr[h, me * cl + j, ri, rk]
            return carry

        lax.fori_loop(0, cl, own, 0)

    def send_dt(k, q):
        ri, rk, i0 = block(q, cols)

        def at(dev):
            return pl.ds(pl.multiple_of(dev * rows + i0, RB), RB)

        for e in range(2):
            scatter(n, me, lambda p, e=e: tr.at[pl.ds(p * cl + e * hc, hc), ri, rk], lambda d, e=e: dt.at[pl.ds(e * hc, hc), at(d), rk], snd(k, e)(q), rcv(k, e)(q))

        def own(j, carry):
            dt[j, at(me), rk] = tr[me * cl + j, ri, rk]
            return carry

        lax.fori_loop(0, cl, own, 0)

    def exchange(product, send, arrived):
        def one(j, carry):
            for e in range(2):
                @pl.when(j == e * hc)
                def _(e=e):
                    arrived(e)

            product(j)
            send(j, 1, 0)
            return carry

        lax.fori_loop(0, cl, one, 0)

        def rest(q, carry):
            send(0, cl, q)
            return carry

        lax.fori_loop(1, nq, rest, 0)

    def exchange_t(k, product, arrived):
        def send(j, count, q):
            ri, rk, i0 = block(q, cols)
            scatter(n, me, lambda p: ts.at[pl.ds(j, count), pl.ds(pl.multiple_of(p * rows + i0, RB), RB), rk], lambda d: tr.at[pl.ds(d * cl + j, count), ri, rk], snd(k)(q), rcv(k)(q))

        exchange(product, send, arrived)

        def own(j, carry):
            tr[me * cl + j, :, :] = ts[j, pl.ds(pl.multiple_of(me * rows, RB), rows), :]
            return carry

        lax.fori_loop(0, cl, own, 0)

    def exchange_dab(k, incoming, ab, arrived):
        def product(j):
            left, right, d_t = ab[0, j], ab[1, j], dt[j]
            if incoming:
                d_left = dot(right, d_t, 1, 1)
                d_right = dot(left, d_t, 1, 0)
            else:
                d_left = dot(d_t, right, 1, 0)
                d_right = dot(d_t, left, 0, 0)
            ab[0, j, :, :] = d_left.astype(BF16)
            ab[1, j, :, :] = d_right.astype(BF16)

        def send(j, count, q):
            ri, rk, i0 = block(q, cols)
            scatter(n, me, lambda p: ab.at[:, pl.ds(j, count), pl.ds(pl.multiple_of(p * rows + i0, RB), RB), rk], lambda d: abr.at[:, pl.ds(d * cl + j, count), ri, rk], snd(k)(q), rcv(k)(q))

        exchange(product, send, arrived)

        def own(j, carry):
            for h in range(2):
                abr[h, me * cl + j, :, :] = ab[h, j, pl.ds(pl.multiple_of(me * rows, RB), rows), :]
            return carry

        lax.fori_loop(0, cl, own, 0)

    load_wpt(0, wp_ref, wpt_v)
    load_mask(m_ref, m_v)
    gain0, shift0 = pair_params(0, lnp_ref)
    gain1, shift1 = pair_params(1, lnp_ref)
    load_z.wait()

    def step1(q, carry):
        ri, rk, i0 = block(q, cols)

        def row(i, carry2):
            r = i0 + i
            xh, _ = norm(get_rows(z_v, r, rk).astype(F32), -1)
            x_row = (xh * gain0 + shift0).astype(BF16)
            put_rows(x_v, r, rk, x_row)
            project(s_ref, i, x_row, get_mask(m_v, r, rk), wpt_v[0], c)
            return carry2

        each_row(row)
        pack_ab(s_ref, c, abr, ri, rk)

        @pl.when(q == 0)
        def _():
            meet(n)

        send_ab(0, q, ab0)
        pltpu.make_async_copy(x_v.at[ri, rk, :], x0_hbm.at[ri, rk, :], osem.at[0]).start()
        return carry

    lax.fori_loop(0, nq, step1, 0)
    load_wpt(1, wp_ref, wpt_v)
    for u in range(2):
        load_chan(u, lnq_ref, gq_v)
    for ref in (gwp, gwg, gwo, glp, glq):
        ref[...] = jnp.zeros_like(ref)
    drain(x_v, osem.at[0])

    def product0(j):
        ts[j, :, :] = dot(ab0[0, j], ab0[1, j], 1, 1).astype(BF16)

    exchange_t(1, product0, lambda e: drain_all(nq, ab_part, rcv(0, e)))
    for e in range(2):
        drain_all(nq, ab_part, snd(0, e))

    def step2(q, carry):
        ri, rk, i0 = block(q, cols)

        @pl.when(q > 0)
        def _():
            drain(t_c, osem.at[1])

        drain(t_part, rcv(1)(q))

        def write_t(sl, val):
            t_c[:, sl, :] = val

        unpack(lambda sl: tr[sl, ri, rk], c, write_t)
        pltpu.make_async_copy(t_c, t0_hbm.at[ri, :, rk], osem.at[1]).start()

        def row(i, carry2):
            r = i0 + i
            th, _ = norm(get_lanes(t_c, i, 0, c), 0)
            y = (th * gq_v[0, 0] + gq_v[0, 1]).astype(BF16)
            upd = dot(y, wo_ref[0], 0, 0)
            gate = jax.nn.sigmoid(dot(get_rows(x_v, r, rk), wg_ref[0], 1, 0))
            z_new = (get_rows(z_v, r, rk).astype(F32) + gate * upd).astype(BF16)
            put_rows(z_v, r, rk, z_new)
            xh, _ = norm(z_new.astype(F32), -1)
            x_row = (xh * gain1 + shift1).astype(BF16)
            put_rows(x_v, r, rk, x_row)
            project(s_ref, i, x_row, get_mask(m_v, r, rk), wpt_v[1], c)
            return carry2

        each_row(row)
        pack_ab(s_ref, c, abr, ri, rk)
        send_ab(2, q, ab1)
        return carry

    lax.fori_loop(0, nq, step2, 0)
    drain(t_c, osem.at[1])
    drain_all(nq, t_part, snd(1))
    load_g.wait()

    def product1(j):
        ts[j, :, :] = dot(ab1[0, j], ab1[1, j], 0, 0).astype(BF16)

    exchange_t(3, product1, lambda e: drain_all(nq, ab_part, rcv(2, e)))
    for e in range(2):
        drain_all(nq, ab_part, snd(2, e))

    def step3(q, carry):
        ri, rk, i0 = block(q, cols)
        drain(t_part, rcv(3)(q))

        def write_t(sl, val):
            t_c[:, sl, :] = val

        unpack(lambda sl: tr[sl, ri, rk], c, write_t)

        @pl.when(q > 0)
        def _():
            drain(zo_c, osem.at[2])

        def row(i, carry2):
            r = i0 + i
            th, rstd = norm(get_lanes(t_c, i, 0, c), 0)
            y = (th * gq_v[1, 0] + gq_v[1, 1]).astype(BF16)
            upd = dot(y, wo_ref[1], 0, 0)
            gate = jax.nn.sigmoid(dot(get_rows(x_v, r, rk), wg_ref[1], 1, 0))
            put_rows(zo_c, i, slice(None), (get_rows(z_v, r, rk).astype(F32) + gate * upd).astype(BF16))
            finish_back(i, r, rk, get_rows(g_v, r, rk).astype(F32), th, rstd, y, upd, gate, gq_v[1, 0], wo_ref[1], dg_v, s_ref, gwo, glq, 1)
            return carry2

        each_row(row)
        pltpu.make_async_copy(zo_c, zo_hbm.at[ri, rk, :], osem.at[2]).start()

        def write(sl, val):
            tr[sl, ri, rk] = val

        pack(s_ref, 0, c, write)
        send_dt(4, q)
        return carry

    lax.fori_loop(0, nq, step3, 0)
    drain(zo_c, osem.at[2])
    exchange_dab(5, True, ab1, lambda e: drain_all(nq, dt_part, rcv(4, e)))
    drain_all(nq, t_part, snd(3))
    for e in range(2):
        drain_all(nq, dt_part, snd(4, e))

    def step4(q, carry):
        ri, rk, i0 = block(q, cols)
        load_t = pltpu.make_async_copy(t0_hbm.at[ri, :, rk], t_c, isem.at[2])
        load_x = pltpu.make_async_copy(x0_hbm.at[ri, rk, :], xp_c, isem.at[3])
        load_t.start()
        load_x.start()
        drain(dab_part, rcv(5)(q))
        unpack_dab(abr, dab_t, c, ri, rk)
        load_t.wait()
        load_x.wait()

        def row(i, carry2):
            r = i0 + i
            dn = project_back(1, i, r, rk, dab_t, m_v, x_v, z_v, dg_v, g_v, gain1, wpt_v, wp_ref, wg_ref, gwp, gwg, glp, c)
            put_rows(g_v, r, rk, dn)
            th, rstd = norm(get_lanes(t_c, i, 0, c), 0)
            y = (th * gq_v[0, 0] + gq_v[0, 1]).astype(BF16)
            upd = dot(y, wo_ref[0], 0, 0)
            gate = jax.nn.sigmoid(dot(get_rows(xp_c, i, slice(None)), wg_ref[0], 1, 0))
            finish_back(i, r, rk, dn.astype(F32), th, rstd, y, upd, gate, gq_v[0, 0], wo_ref[0], dg_v, s_ref, gwo, glq, 0)
            return carry2

        each_row(row)

        def write(sl, val):
            tr[sl, ri, rk] = val

        pack(s_ref, 0, c, write)
        send_dt(6, q)
        return carry

    lax.fori_loop(0, nq, step4, 0)
    reload_z = pltpu.make_async_copy(z_hbm, z_v, isem.at[0])
    reload_x = pltpu.make_async_copy(x0_hbm, x_v, isem.at[1])
    reload_z.start()
    reload_x.start()
    small = [jnp.sum(glp[1, h], axis=0, keepdims=True) for h in range(2)]
    small += [jnp.sum(glq[u, h].T, axis=0, keepdims=True) for u in (1, 0) for h in range(2)]
    small = jnp.concatenate(small + [jnp.zeros((2, c), F32)], axis=0)
    e1, e2, e3, e4 = we, we + wc, we + 2 * wc, we + 3 * wc

    def fill(p, carry):
        z, k = p // 2, lax.rem(p, 2)
        cut = pl.ds(pl.multiple_of(p * wc, 8), wc)
        early[z, k, 0:e1, :] = gwp[1, pl.ds(pl.multiple_of(p * we, 8), we), :]
        early[z, k, e1:e2, :] = gwg[1, cut, :]
        early[z, k, e2:e3, :] = gwo[1, cut, :]
        early[z, k, e3:e4, :] = gwo[0, cut, :]
        early[z, k, e4:e4 + 8, :] = small
        return carry

    lax.fori_loop(0, n, fill, 0)
    to_pair(n, me, early.at[:, 1 - core], pair_e, gss.at[0], grs.at[0])
    exchange_dab(7, False, ab0, lambda e: drain_all(nq, dt_part, rcv(6, e)))
    drain_all(nq, dab_part, snd(5))
    for e in range(2):
        drain_all(nq, dt_part, snd(6, e))
    drain(pair_e, grs.at[0])
    pair_sum(core, early, pair_e, comb_e)
    gath_e[chip] = comb_e[chip]
    to_chips(n, me, lambda o: comb_e.at[o], lambda d: gath_e.at[d], gss.at[1], grs.at[1])
    reload_z.wait()
    reload_x.wait()

    def step5(q, carry):
        ri, rk, i0 = block(q, cols)
        drain(dab_part, rcv(7)(q))
        unpack_dab(abr, dab_t, c, ri, rk)

        def row(i, carry2):
            r = i0 + i
            dn = project_back(0, i, r, rk, dab_t, m_v, x_v, z_v, dg_v, g_v, gain0, wpt_v, wp_ref, wg_ref, gwp, gwg, glp, c)
            put_rows(g_v, r, rk, dn)
            return carry2

        each_row(row)
        pltpu.make_async_copy(g_v.at[ri, rk, :], dz_hbm.at[ri, rk, :], osem.at[3]).start()
        return carry

    lax.fori_loop(0, nq, step5, 0)
    tail = jnp.concatenate([jnp.sum(glp[0, h], axis=0, keepdims=True) for h in range(2)] + [jnp.zeros((6, c), F32)], axis=0)

    def fill_late(p, carry):
        z, k = p // 2, lax.rem(p, 2)
        late[z, k, 0:e1, :] = gwp[0, pl.ds(pl.multiple_of(p * we, 8), we), :]
        late[z, k, e1:e2, :] = gwg[0, pl.ds(pl.multiple_of(p * wc, 8), wc), :]
        late[z, k, e2:e2 + 8, :] = tail
        return carry

    lax.fori_loop(0, n, fill_late, 0)
    to_pair(n, me, late.at[:, 1 - core], pair_l, gss.at[2], grs.at[2])
    drain(gath_e.at[pl.ds(0, n // 2 - 1)], grs.at[1])
    sum_e = add_parts(gath_e)
    drain(pair_l, grs.at[2])
    pair_sum(core, late, pair_l, comb_l)
    gath_l[chip] = comb_l[chip]
    to_chips(n, me, lambda o: comb_l.at[o], lambda d: gath_l.at[d], gss.at[3], grs.at[3])
    drain(gath_l.at[pl.ds(0, n // 2 - 1)], grs.at[3])
    sum_l = add_parts(gath_l)
    mine[...] = jnp.concatenate([sum_e[0:e1], sum_l[0:e1], sum_e[e1:e4], sum_l[e1:e2]], axis=0).astype(BF16)
    to_chips(n, me, lambda o: mine, lambda d: all_v.at[core, d], gss.at[4], grs.at[4])
    all_v[core, chip] = mine[...]
    small_ref[0:8, :] = sum_e[e4:e4 + 8]
    small_ref[8:16, :] = sum_l[e2:e2 + 8]
    drain(dz_hbm, osem.at[3])
    drain_all(nq, dab_part, snd(7))
    drain(pair_e, gss.at[0])
    drain(gath_e.at[pl.ds(0, n // 2 - 1)], gss.at[1])
    drain(pair_l, gss.at[2])
    drain(gath_l.at[pl.ds(0, n // 2 - 1)], gss.at[3])
    others = all_v.at[0, pl.ds(0, n // 2 - 1)]
    drain(others, gss.at[4])
    drain(others, grs.at[4])
    to_pair(n, me, all_v.at[core], all_v.at[core], gss.at[5], grs.at[5])
    drain(all_v.at[core], gss.at[5])
    drain(all_v.at[1 - core], grs.at[5])
    grads_ref[...] = all_v[...]


def solution(mesh):
    row_spec = P(('data', AXIS), None, None)
    mask_spec = P(('data', AXIS), None)
    grad_spec = P('data', None, None)
    n = mesh.shape[AXIS]

    def device_step(z0, mask, g, ln_pair, w_proj, w_gate, ln_chan, w_out):
        rows, cols, c = z0.shape
        cl = c // n
        nq = (rows // RB) * (cols // KB)
        we, wc = 4 * c // n, c // n
        er, lr, gr = we + 3 * wc + 8, we + wc + 8, 2 * we + 4 * wc
        half = n // 2
        vm = pltpu.VMEM
        dma = pltpu.SemaphoreType.DMA
        row_t = jax.ShapeDtypeStruct((rows, cols, c), BF16)
        row_v = vm((rows, cols, c), BF16)
        chan_v = vm((cl, cols, cols), BF16)
        scratch = [vm((2, cl, cols, cols), BF16)] * 2 + [vm((2, c, rows, cols), BF16), chan_v, vm((c, rows, cols), BF16), chan_v] + [row_v] * 4
        scratch += [vm((RB, 2 * c, KB), F32), vm((RB, 2 * c, KB), BF16), vm((RB, c, KB), BF16), vm((RB, KB, c), BF16), vm((RB, KB, c), BF16)]
        scratch += [vm((2, 4 * c, c), BF16), vm((2, 2, c, 2 * KB), F32), vm((rows, 1, cols), F32)]
        scratch += [vm((2, 4 * c, c), F32), vm((2, c, c), F32), vm((2, c, c), F32), vm((2, 2, 8, c), F32), vm((2, 2, c, 128), F32)]
        for k in (er, lr):
            scratch += [vm((half, 2, k, c), F32)] + [vm((half, k, c), F32)] * 3
        scratch += [vm((gr, c), BF16), vm((2, half, gr, c), BF16)]
        scratch += [dma((8, 2, 2, nq)), dma((4,)), dma((4,)), dma((6,)), dma((6,))]
        z2, dz, _, _, grads, small = pl.pallas_call(
            functools.partial(whole_kernel, n),
            out_shape=(row_t, row_t, row_t, jax.ShapeDtypeStruct((rows, c, cols), BF16), jax.ShapeDtypeStruct((2, half, gr, c), BF16), jax.ShapeDtypeStruct((16, c), F32)),
            in_specs=[ANY, VM, ANY] + [VM] * 5,
            out_specs=(ANY, ANY, ANY, ANY, VM, VM),
            scratch_shapes=scratch,
            compiler_params=pltpu.CompilerParams(collective_id=1, has_side_effects=True, vmem_limit_bytes=67043328),
            name='whole',
        )(z0, mask, g, ln_pair, w_proj, w_gate, ln_chan, w_out)

        def rows_of(start, count):
            return jnp.swapaxes(grads[:, :, start:start + count], 0, 1).reshape(n * count, c)

        base = 2 * we
        d_wp = jnp.stack([rows_of(we, we).T, rows_of(0, we).T])
        d_wg = jnp.stack([rows_of(base + 3 * wc, wc), rows_of(base, wc)])
        d_wo = jnp.stack([rows_of(base + 2 * wc, wc), rows_of(base + wc, wc)])
        small = small.astype(BF16)
        d_lp = jnp.stack([small[8:10], small[0:2]])
        d_lq = jnp.stack([small[4:6], small[2:4]])
        return z2, dz, d_lp, d_wp, d_wg, d_lq, d_wo

    full = P()
    return jax.shard_map(device_step, mesh=mesh, in_specs=(row_spec, mask_spec, row_spec, full, full, full, full, full), out_specs=(row_spec, row_spec, grad_spec, grad_spec, grad_spec, grad_spec, grad_spec), check_vma=False)
```

```python
import functools

import jax
import jax.numpy as jnp
from jax import lax
from jax.experimental import pallas as pl
from jax.experimental.pallas import tpu as pltpu
from jax.sharding import PartitionSpec as P

LN_EPS = 1e-5
AXIS = 'dap'
F32 = jnp.float32
BF16 = jnp.bfloat16
RB = 16
KB = 128
UNROLL = 2
MESH_ID = pl.DeviceIdType.MESH
ANY = pl.BlockSpec(memory_space=pl.ANY)
VM = pl.BlockSpec(memory_space=pltpu.VMEM)


def dot(lhs, rhs, lc, rc):
    return lax.dot_general(lhs, rhs, (((lc,), (rc,)), ((), ())), preferred_element_type=F32)


def norm(values, axis):
    mean = jnp.mean(values, axis=axis, keepdims=True)
    cent = values - mean
    var = jnp.mean(cent * cent, axis=axis, keepdims=True)
    rstd = lax.rsqrt(var + LN_EPS)
    return cent * rstd, rstd


def greet(n):
    me = lax.axis_index(AXIS)
    bar = pltpu.get_barrier_semaphore()

    def one(s, carry):
        pl.semaphore_signal(bar, inc=1, device_id={AXIS: lax.rem(me + s, n)}, device_id_type=MESH_ID)
        return carry

    lax.fori_loop(1, n, one, 0)
    return me


def meet(n):
    pl.semaphore_wait(pltpu.get_barrier_semaphore(), n - 1)


def scatter(n, me, src, dst, ssem, rsem):
    def one(s, carry):
        far = (s + 1) // 2
        peer = lax.rem(me + far * lax.rem(s, 2) + (n - far) * (1 - lax.rem(s, 2)), n)
        pltpu.make_async_remote_copy(src_ref=src(peer), dst_ref=dst(me), send_sem=ssem, recv_sem=rsem, device_id={AXIS: peer}, device_id_type=MESH_ID).start()
        return carry

    lax.fori_loop(1, n, one, 0)


def drain(ref, sem):
    pltpu.make_async_copy(ref, ref, sem).wait()


def drain_all(nq, part, sem):
    def one(q, carry):
        drain(part, sem(q))
        return carry

    lax.fori_loop(0, nq, one, 0)


def block(q, cols):
    per = cols // KB
    i0 = pl.multiple_of((q // per) * RB, RB)
    k0 = pl.multiple_of(lax.rem(q, per) * KB, KB)
    return pl.ds(i0, RB), pl.ds(k0, KB), i0


def pair_params(u, lnp_ref):
    return lnp_ref[u, 0:1, :].astype(F32), lnp_ref[u, 1:2, :].astype(F32)


def load_wpt(u, wp_ref, wpt_v):
    wpt_v[u] = wp_ref[u].astype(F32).T.astype(BF16)


def load_mask(m_ref, m_v):
    for r in range(m_v.shape[0]):
        m_v[r, 0:1, :] = m_ref[r:r + 1, :].astype(F32)


def load_chan(u, lnq_ref, gq_v):
    c = gq_v.shape[2]
    for h in range(2):
        row = lnq_ref[u, h:h + 1, :].astype(F32)
        col = jnp.broadcast_to(row, (128, c)).T
        for l in range(gq_v.shape[3] // 128):
            gq_v[u, h, :, l * 128:(l + 1) * 128] = col


def pack(s_ref, e0, count, write):
    def one(e, carry):
        off = pl.multiple_of(e * 8, 8)
        val = s_ref[:, pl.ds(e0 + off, 8), :]
        write(pl.ds(off, 8), jnp.swapaxes(val, 0, 1).astype(BF16))
        return carry

    lax.fori_loop(0, count // 8, one, 0)


def unpack(read, count, write):
    def one(e, carry):
        sl = pl.ds(pl.multiple_of(e * 16, 16), 16)
        write(sl, jnp.swapaxes(read(sl).astype(F32), 0, 1).astype(BF16))
        return carry

    lax.fori_loop(0, count // 16, one, 0)


def each_row(row):
    def pair(k, carry):
        return row(2 * k, carry)

    lax.fori_loop(0, RB // 2, pair, 0, unroll=UNROLL)


def get_rows(ref, r, rk):
    return ref[pl.ds(r, 2), rk, :].reshape(2 * KB, ref.shape[2])


def put_rows(ref, r, rk, val):
    ref[pl.ds(r, 2), rk, :] = val.reshape(2, KB, val.shape[1])


def get_lanes(ref, i, lo, hi):
    return jnp.concatenate([ref[i, lo:hi, :].astype(F32), ref[i + 1, lo:hi, :].astype(F32)], axis=1)


def put_lanes(ref, i, lo, hi, val):
    ref[i, lo:hi, :] = val[:, :KB]
    ref[i + 1, lo:hi, :] = val[:, KB:]


def get_mask(m_v, r, rk):
    return jnp.concatenate([m_v[r, 0:1, rk], m_v[r + 1, 0:1, rk]], axis=1)


def project(s_ref, i, x_row, m_row, w_t, c):
    p = dot(w_t, x_row, 1, 1)
    put_lanes(s_ref, i, 0, c, m_row * jax.nn.sigmoid(p[c:2 * c]) * p[0:c])
    put_lanes(s_ref, i, c, 2 * c, m_row * jax.nn.sigmoid(p[3 * c:]) * p[2 * c:3 * c])


def fold_rows(v):
    return jnp.sum(v.reshape(v.shape[0] // 8, 8, v.shape[1]), axis=0)


def fold_lanes(v):
    out = v[:, 0:128]
    for h in range(1, v.shape[1] // 128):
        out = out + v[:, h * 128:(h + 1) * 128]
    return out


def pack_ab(s_ref, c, abr, ri, rk):
    for h in range(2):
        def write(sl, val, h=h):
            abr[h, sl, ri, rk] = val
        pack(s_ref, h * c, c, write)


def unpack_dab(abr, dab_t, c, ri, rk):
    for h in range(2):
        def write_t(sl, val, h=h):
            dab_t[:, pl.ds(pl.multiple_of(h * c + sl.start, 16), 16), :] = val
        unpack(lambda sl, h=h: abr[h, sl, ri, rk], c, write_t)


def finish_back(i, r, rk, dn, th, rstd, y, upd, gate, gain, w_out, dg_v, s_ref, gwo, glq, u):
    d_gate = dn * upd * gate * (1.0 - gate)
    d_upd = (dn * gate).astype(BF16)
    put_rows(dg_v, r, rk, d_gate.astype(BF16))
    gwo[u] += dot(y, d_upd, 1, 0)
    dy = dot(w_out, d_upd, 1, 1).astype(BF16).astype(F32)
    glq[u, 0] += fold_lanes(dy * th)
    glq[u, 1] += fold_lanes(dy)
    dyg = dy * gain
    m1 = jnp.mean(dyg, axis=0, keepdims=True)
    m2 = jnp.mean(dyg * th, axis=0, keepdims=True)
    put_lanes(s_ref, i, 0, dy.shape[0], rstd * (dyg - m1 - th * m2))


def project_back(u, i, r, rk, dab_t, m_v, x_v, z_v, dg_v, dn_v, gain, wpt_v, wp_ref, wg_ref, gwp, gwg, glp, c):
    x_row = get_rows(x_v, r, rk)
    m_row = get_mask(m_v, r, rk)
    p = dot(wpt_v[u], x_row, 1, 1)
    parts = []
    for h in range(2):
        d_val = get_lanes(dab_t, i, h * c, (h + 1) * c) * m_row
        lin = p[2 * h * c:(2 * h + 1) * c]
        sig = jax.nn.sigmoid(p[(2 * h + 1) * c:(2 * h + 2) * c])
        d_lin = d_val * sig
        parts.append(d_lin.astype(BF16))
        parts.append((d_lin * lin * (1.0 - sig)).astype(BF16))
    d_proj = jnp.concatenate(parts, axis=0)
    d_gate = get_rows(dg_v, r, rk)
    gwp[u] += dot(d_proj, x_row, 1, 0)
    gwg[u] += dot(x_row, d_gate, 0, 0)
    dxt = dot(wp_ref[u], d_proj, 1, 0) + dot(wg_ref[u], d_gate, 1, 1)
    dx = dxt.T.astype(BF16).astype(F32)
    xh, rstd = norm(get_rows(z_v, r, rk).astype(F32), -1)
    glp[u, 0] += fold_rows(dx * xh)
    glp[u, 1] += fold_rows(dx)
    dxg = dx * gain
    m1 = jnp.mean(dxg, axis=-1, keepdims=True)
    m2 = jnp.mean(dxg * xh, axis=-1, keepdims=True)
    return (get_rows(dn_v, r, rk).astype(F32) + rstd * (dxg - m1 - xh * m2)).astype(BF16)


def to_pair(n, me, src, dst, ssem, rsem):
    partner = me + 1 - 2 * lax.rem(me, 2)
    pltpu.make_async_remote_copy(src_ref=src, dst_ref=dst, send_sem=ssem, recv_sem=rsem, device_id={AXIS: partner}, device_id_type=MESH_ID).start()


def to_chips(n, me, src, dst, ssem, rsem):
    core, chip = lax.rem(me, 2), me // 2

    def one(s, carry):
        other = lax.rem(chip + s, n // 2)
        pltpu.make_async_remote_copy(src_ref=src(other), dst_ref=dst(chip), send_sem=ssem, recv_sem=rsem, device_id={AXIS: 2 * other + core}, device_id_type=MESH_ID).start()
        return carry

    lax.fori_loop(1, n // 2, one, 0)


def pair_sum(core, parts, pair_in, comb):
    def one(z, carry):
        comb[z] = parts[z, core] + pair_in[z]
        return carry

    lax.fori_loop(0, comb.shape[0], one, 0)


def add_parts(recv):
    def one(s, acc):
        return acc + recv[s]

    return lax.fori_loop(1, recv.shape[0], one, recv[0])


def whole_kernel(n, z_hbm, m_ref, g_hbm, lnp_ref, wp_ref, wg_ref, lnq_ref, wo_ref,
                 zo_hbm, dz_hbm, x0_hbm, t0_hbm, grads_ref, small_ref,
                 ab0, ab1, abr, ts, tr, dt, z_v, x_v, g_v, dg_v, s_ref, dab_t, t_c, xp_c, zo_c,
                 wpt_v, gq_v, m_v, gwp, gwg, gwo, glp, glq,
                 early, pair_e, comb_e, gath_e, late, pair_l, comb_l, gath_l, mine, all_v,
                 sems, isem, osem, gss, grs):
    rows, cols, c = z_v.shape
    cl = c // n
    nq = (rows // RB) * (cols // KB)
    we, wc = 4 * c // n, c // n
    load_z = pltpu.make_async_copy(z_hbm, z_v, isem.at[0])
    load_g = pltpu.make_async_copy(g_hbm, g_v, isem.at[1])
    load_z.start()
    load_g.start()
    me = greet(n)
    core, chip = lax.rem(me, 2), me // 2

    def snd(k, h=0):
        return lambda q: sems.at[k, h, 0, q]

    def rcv(k, h=0):
        return lambda q: sems.at[k, h, 1, q]

    hc = cl // 2

    ab_part = ab0.at[:, pl.ds(0, cl // 2), pl.ds(0, RB * (n - 1)), pl.ds(0, KB)]
    dt_part = dt.at[pl.ds(0, cl // 2), pl.ds(0, RB * (n - 1)), pl.ds(0, KB)]
    t_part = tr.at[pl.ds(0, c - cl), pl.ds(0, RB), pl.ds(0, KB)]
    dab_part = abr.at[:, pl.ds(0, c - cl), pl.ds(0, RB), pl.ds(0, KB)]

    def send_ab(k, q, dest):
        ri, rk, i0 = block(q, cols)

        def at(dev):
            return pl.ds(pl.multiple_of(dev * rows + i0, RB), RB)

        for e in range(2):
            scatter(n, me, lambda p, e=e: abr.at[:, pl.ds(p * cl + e * hc, hc), ri, rk], lambda d, e=e: dest.at[:, pl.ds(e * hc, hc), at(d), rk], snd(k, e)(q), rcv(k, e)(q))

        def own(j, carry):
            for h in range(2):
                dest[h, j, at(me), rk] = abr[h, me * cl + j, ri, rk]
            return carry

        lax.fori_loop(0, cl, own, 0)

    def send_dt(k, q):
        ri, rk, i0 = block(q, cols)

        def at(dev):
            return pl.ds(pl.multiple_of(dev * rows + i0, RB), RB)

        for e in range(2):
            scatter(n, me, lambda p, e=e: tr.at[pl.ds(p * cl + e * hc, hc), ri, rk], lambda d, e=e: dt.at[pl.ds(e * hc, hc), at(d), rk], snd(k, e)(q), rcv(k, e)(q))

        def own(j, carry):
            dt[j, at(me), rk] = tr[me * cl + j, ri, rk]
            return carry

        lax.fori_loop(0, cl, own, 0)

    def exchange(product, send, arrived, batch):
        def one(j, carry):
            product(j)
            return carry

        def some(b, carry):
            j0 = b * batch
            for e in range(2):
                @pl.when(j0 == e * hc)
                def _(e=e):
                    arrived(e)

            lax.fori_loop(j0, j0 + batch, one, 0)
            send(j0, batch, 0)
            return carry

        lax.fori_loop(0, cl // batch, some, 0)

        def rest(q, carry):
            send(0, cl, q)
            return carry

        lax.fori_loop(1, nq, rest, 0)

    def exchange_t(k, product, arrived):
        def send(j, count, q):
            ri, rk, i0 = block(q, cols)
            scatter(n, me, lambda p: ts.at[pl.ds(j, count), pl.ds(pl.multiple_of(p * rows + i0, RB), RB), rk], lambda d: tr.at[pl.ds(d * cl + j, count), ri, rk], snd(k)(q), rcv(k)(q))

        exchange(product, send, arrived, hc)

        def own(j, carry):
            tr[me * cl + j, :, :] = ts[j, pl.ds(pl.multiple_of(me * rows, RB), rows), :]
            return carry

        lax.fori_loop(0, cl, own, 0)

    def exchange_dab(k, incoming, ab, arrived):
        def product(j):
            left, right, d_t = ab[0, j], ab[1, j], dt[j]
            if incoming:
                d_left = dot(right, d_t, 1, 1)
                d_right = dot(left, d_t, 1, 0)
            else:
                d_left = dot(d_t, right, 1, 0)
                d_right = dot(d_t, left, 0, 0)
            ab[0, j, :, :] = d_left.astype(BF16)
            ab[1, j, :, :] = d_right.astype(BF16)

        def send(j, count, q):
            ri, rk, i0 = block(q, cols)
            scatter(n, me, lambda p: ab.at[:, pl.ds(j, count), pl.ds(pl.multiple_of(p * rows + i0, RB), RB), rk], lambda d: abr.at[:, pl.ds(d * cl + j, count), ri, rk], snd(k)(q), rcv(k)(q))

        exchange(product, send, arrived, hc // 2)

        def own(j, carry):
            for h in range(2):
                abr[h, me * cl + j, :, :] = ab[h, j, pl.ds(pl.multiple_of(me * rows, RB), rows), :]
            return carry

        lax.fori_loop(0, cl, own, 0)

    load_wpt(0, wp_ref, wpt_v)
    load_mask(m_ref, m_v)
    gain0, shift0 = pair_params(0, lnp_ref)
    gain1, shift1 = pair_params(1, lnp_ref)
    load_z.wait()

    def step1(q, carry):
        ri, rk, i0 = block(q, cols)

        def row(i, carry2):
            r = i0 + i
            xh, _ = norm(get_rows(z_v, r, rk).astype(F32), -1)
            x_row = (xh * gain0 + shift0).astype(BF16)
            put_rows(x_v, r, rk, x_row)
            project(s_ref, i, x_row, get_mask(m_v, r, rk), wpt_v[0], c)
            return carry2

        each_row(row)
        pack_ab(s_ref, c, abr, ri, rk)

        @pl.when(q == 0)
        def _():
            meet(n)

        send_ab(0, q, ab0)
        pltpu.make_async_copy(x_v.at[ri, rk, :], x0_hbm.at[ri, rk, :], osem.at[0]).start()
        return carry

    lax.fori_loop(0, nq, step1, 0)
    load_wpt(1, wp_ref, wpt_v)
    for u in range(2):
        load_chan(u, lnq_ref, gq_v)
    for ref in (gwp, gwg, gwo, glp, glq):
        ref[...] = jnp.zeros_like(ref)
    drain(x_v, osem.at[0])

    def product0(j):
        ts[j, :, :] = dot(ab0[0, j], ab0[1, j], 1, 1).astype(BF16)

    exchange_t(1, product0, lambda e: drain_all(nq, ab_part, rcv(0, e)))
    for e in range(2):
        drain_all(nq, ab_part, snd(0, e))

    def step2(q, carry):
        ri, rk, i0 = block(q, cols)

        @pl.when(q > 0)
        def _():
            drain(t_c, osem.at[1])

        drain(t_part, rcv(1)(q))

        def write_t(sl, val):
            t_c[:, sl, :] = val

        unpack(lambda sl: tr[sl, ri, rk], c, write_t)
        pltpu.make_async_copy(t_c, t0_hbm.at[ri, :, rk], osem.at[1]).start()

        def row(i, carry2):
            r = i0 + i
            th, _ = norm(get_lanes(t_c, i, 0, c), 0)
            y = (th * gq_v[0, 0] + gq_v[0, 1]).astype(BF16)
            upd = dot(y, wo_ref[0], 0, 0)
            gate = jax.nn.sigmoid(dot(get_rows(x_v, r, rk), wg_ref[0], 1, 0))
            z_new = (get_rows(z_v, r, rk).astype(F32) + gate * upd).astype(BF16)
            put_rows(z_v, r, rk, z_new)
            xh, _ = norm(z_new.astype(F32), -1)
            x_row = (xh * gain1 + shift1).astype(BF16)
            put_rows(x_v, r, rk, x_row)
            project(s_ref, i, x_row, get_mask(m_v, r, rk), wpt_v[1], c)
            return carry2

        each_row(row)
        pack_ab(s_ref, c, abr, ri, rk)
        send_ab(2, q, ab1)
        return carry

    lax.fori_loop(0, nq, step2, 0)
    drain(t_c, osem.at[1])
    drain_all(nq, t_part, snd(1))
    load_g.wait()

    def product1(j):
        ts[j, :, :] = dot(ab1[0, j], ab1[1, j], 0, 0).astype(BF16)

    exchange_t(3, product1, lambda e: drain_all(nq, ab_part, rcv(2, e)))
    for e in range(2):
        drain_all(nq, ab_part, snd(2, e))

    def step3(q, carry):
        ri, rk, i0 = block(q, cols)
        drain(t_part, rcv(3)(q))

        def write_t(sl, val):
            t_c[:, sl, :] = val

        unpack(lambda sl: tr[sl, ri, rk], c, write_t)

        @pl.when(q > 0)
        def _():
            drain(zo_c, osem.at[2])

        def row(i, carry2):
            r = i0 + i
            th, rstd = norm(get_lanes(t_c, i, 0, c), 0)
            y = (th * gq_v[1, 0] + gq_v[1, 1]).astype(BF16)
            upd = dot(y, wo_ref[1], 0, 0)
            gate = jax.nn.sigmoid(dot(get_rows(x_v, r, rk), wg_ref[1], 1, 0))
            put_rows(zo_c, i, slice(None), (get_rows(z_v, r, rk).astype(F32) + gate * upd).astype(BF16))
            finish_back(i, r, rk, get_rows(g_v, r, rk).astype(F32), th, rstd, y, upd, gate, gq_v[1, 0], wo_ref[1], dg_v, s_ref, gwo, glq, 1)
            return carry2

        each_row(row)
        pltpu.make_async_copy(zo_c, zo_hbm.at[ri, rk, :], osem.at[2]).start()

        def write(sl, val):
            tr[sl, ri, rk] = val

        pack(s_ref, 0, c, write)
        send_dt(4, q)
        return carry

    lax.fori_loop(0, nq, step3, 0)
    drain(zo_c, osem.at[2])
    exchange_dab(5, True, ab1, lambda e: drain_all(nq, dt_part, rcv(4, e)))
    drain_all(nq, t_part, snd(3))
    for e in range(2):
        drain_all(nq, dt_part, snd(4, e))

    def step4(q, carry):
        ri, rk, i0 = block(q, cols)
        load_t = pltpu.make_async_copy(t0_hbm.at[ri, :, rk], t_c, isem.at[2])
        load_x = pltpu.make_async_copy(x0_hbm.at[ri, rk, :], xp_c, isem.at[3])
        load_t.start()
        load_x.start()
        drain(dab_part, rcv(5)(q))
        unpack_dab(abr, dab_t, c, ri, rk)
        load_t.wait()
        load_x.wait()

        def row(i, carry2):
            r = i0 + i
            dn = project_back(1, i, r, rk, dab_t, m_v, x_v, z_v, dg_v, g_v, gain1, wpt_v, wp_ref, wg_ref, gwp, gwg, glp, c)
            put_rows(g_v, r, rk, dn)
            th, rstd = norm(get_lanes(t_c, i, 0, c), 0)
            y = (th * gq_v[0, 0] + gq_v[0, 1]).astype(BF16)
            upd = dot(y, wo_ref[0], 0, 0)
            gate = jax.nn.sigmoid(dot(get_rows(xp_c, i, slice(None)), wg_ref[0], 1, 0))
            finish_back(i, r, rk, dn.astype(F32), th, rstd, y, upd, gate, gq_v[0, 0], wo_ref[0], dg_v, s_ref, gwo, glq, 0)
            return carry2

        each_row(row)

        def write(sl, val):
            tr[sl, ri, rk] = val

        pack(s_ref, 0, c, write)
        send_dt(6, q)
        return carry

    lax.fori_loop(0, nq, step4, 0)
    reload_z = pltpu.make_async_copy(z_hbm, z_v, isem.at[0])
    reload_x = pltpu.make_async_copy(x0_hbm, x_v, isem.at[1])
    reload_z.start()
    reload_x.start()
    small = [jnp.sum(glp[1, h], axis=0, keepdims=True) for h in range(2)]
    small += [jnp.sum(glq[u, h].T, axis=0, keepdims=True) for u in (1, 0) for h in range(2)]
    small = jnp.concatenate(small + [jnp.zeros((2, c), F32)], axis=0)
    e1, e2, e3, e4 = we, we + wc, we + 2 * wc, we + 3 * wc

    def fill(p, carry):
        z, k = p // 2, lax.rem(p, 2)
        cut = pl.ds(pl.multiple_of(p * wc, 8), wc)
        early[z, k, 0:e1, :] = gwp[1, pl.ds(pl.multiple_of(p * we, 8), we), :]
        early[z, k, e1:e2, :] = gwg[1, cut, :]
        early[z, k, e2:e3, :] = gwo[1, cut, :]
        early[z, k, e3:e4, :] = gwo[0, cut, :]
        early[z, k, e4:e4 + 8, :] = small
        return carry

    lax.fori_loop(0, n, fill, 0)
    to_pair(n, me, early.at[:, 1 - core], pair_e, gss.at[0], grs.at[0])
    exchange_dab(7, False, ab0, lambda e: drain_all(nq, dt_part, rcv(6, e)))
    drain_all(nq, dab_part, snd(5))
    for e in range(2):
        drain_all(nq, dt_part, snd(6, e))
    drain(pair_e, grs.at[0])
    pair_sum(core, early, pair_e, comb_e)
    gath_e[chip] = comb_e[chip]
    to_chips(n, me, lambda o: comb_e.at[o], lambda d: gath_e.at[d], gss.at[1], grs.at[1])
    reload_z.wait()
    reload_x.wait()

    def step5(q, carry):
        ri, rk, i0 = block(q, cols)
        drain(dab_part, rcv(7)(q))
        unpack_dab(abr, dab_t, c, ri, rk)

        def row(i, carry2):
            r = i0 + i
            dn = project_back(0, i, r, rk, dab_t, m_v, x_v, z_v, dg_v, g_v, gain0, wpt_v, wp_ref, wg_ref, gwp, gwg, glp, c)
            put_rows(g_v, r, rk, dn)
            return carry2

        each_row(row)
        pltpu.make_async_copy(g_v.at[ri, rk, :], dz_hbm.at[ri, rk, :], osem.at[3]).start()
        return carry

    lax.fori_loop(0, nq, step5, 0)
    tail = jnp.concatenate([jnp.sum(glp[0, h], axis=0, keepdims=True) for h in range(2)] + [jnp.zeros((6, c), F32)], axis=0)

    def fill_late(p, carry):
        z, k = p // 2, lax.rem(p, 2)
        late[z, k, 0:e1, :] = gwp[0, pl.ds(pl.multiple_of(p * we, 8), we), :]
        late[z, k, e1:e2, :] = gwg[0, pl.ds(pl.multiple_of(p * wc, 8), wc), :]
        late[z, k, e2:e2 + 8, :] = tail
        return carry

    lax.fori_loop(0, n, fill_late, 0)
    to_pair(n, me, late.at[:, 1 - core], pair_l, gss.at[2], grs.at[2])
    drain(gath_e.at[pl.ds(0, n // 2 - 1)], grs.at[1])
    sum_e = add_parts(gath_e)
    drain(pair_l, grs.at[2])
    pair_sum(core, late, pair_l, comb_l)
    gath_l[chip] = comb_l[chip]
    to_chips(n, me, lambda o: comb_l.at[o], lambda d: gath_l.at[d], gss.at[3], grs.at[3])
    drain(gath_l.at[pl.ds(0, n // 2 - 1)], grs.at[3])
    sum_l = add_parts(gath_l)
    mine[...] = jnp.concatenate([sum_e[0:e1], sum_l[0:e1], sum_e[e1:e4], sum_l[e1:e2]], axis=0).astype(BF16)
    to_chips(n, me, lambda o: mine, lambda d: all_v.at[core, d], gss.at[4], grs.at[4])
    all_v[core, chip] = mine[...]
    small_ref[0:8, :] = sum_e[e4:e4 + 8]
    small_ref[8:16, :] = sum_l[e2:e2 + 8]
    drain(dz_hbm, osem.at[3])
    drain_all(nq, dab_part, snd(7))
    drain(pair_e, gss.at[0])
    drain(gath_e.at[pl.ds(0, n // 2 - 1)], gss.at[1])
    drain(pair_l, gss.at[2])
    drain(gath_l.at[pl.ds(0, n // 2 - 1)], gss.at[3])
    others = all_v.at[0, pl.ds(0, n // 2 - 1)]
    drain(others, gss.at[4])
    drain(others, grs.at[4])
    to_pair(n, me, all_v.at[core], all_v.at[core], gss.at[5], grs.at[5])
    drain(all_v.at[core], gss.at[5])
    drain(all_v.at[1 - core], grs.at[5])
    grads_ref[...] = all_v[...]


def solution(mesh):
    row_spec = P(('data', AXIS), None, None)
    mask_spec = P(('data', AXIS), None)
    grad_spec = P('data', None, None)
    n = mesh.shape[AXIS]

    def device_step(z0, mask, g, ln_pair, w_proj, w_gate, ln_chan, w_out):
        rows, cols, c = z0.shape
        cl = c // n
        nq = (rows // RB) * (cols // KB)
        we, wc = 4 * c // n, c // n
        er, lr, gr = we + 3 * wc + 8, we + wc + 8, 2 * we + 4 * wc
        half = n // 2
        vm = pltpu.VMEM
        dma = pltpu.SemaphoreType.DMA
        row_t = jax.ShapeDtypeStruct((rows, cols, c), BF16)
        row_v = vm((rows, cols, c), BF16)
        chan_v = vm((cl, cols, cols), BF16)
        scratch = [vm((2, cl, cols, cols), BF16)] * 2 + [vm((2, c, rows, cols), BF16), chan_v, vm((c, rows, cols), BF16), chan_v] + [row_v] * 4
        scratch += [vm((RB, 2 * c, KB), F32), vm((RB, 2 * c, KB), BF16), vm((RB, c, KB), BF16), vm((RB, KB, c), BF16), vm((RB, KB, c), BF16)]
        scratch += [vm((2, 4 * c, c), BF16), vm((2, 2, c, 2 * KB), F32), vm((rows, 1, cols), F32)]
        scratch += [vm((2, 4 * c, c), F32), vm((2, c, c), F32), vm((2, c, c), F32), vm((2, 2, 8, c), F32), vm((2, 2, c, 128), F32)]
        for k in (er, lr):
            scratch += [vm((half, 2, k, c), F32)] + [vm((half, k, c), F32)] * 3
        scratch += [vm((gr, c), BF16), vm((2, half, gr, c), BF16)]
        scratch += [dma((8, 2, 2, nq)), dma((4,)), dma((4,)), dma((6,)), dma((6,))]
        z2, dz, _, _, grads, small = pl.pallas_call(
            functools.partial(whole_kernel, n),
            out_shape=(row_t, row_t, row_t, jax.ShapeDtypeStruct((rows, c, cols), BF16), jax.ShapeDtypeStruct((2, half, gr, c), BF16), jax.ShapeDtypeStruct((16, c), F32)),
            in_specs=[ANY, VM, ANY] + [VM] * 5,
            out_specs=(ANY, ANY, ANY, ANY, VM, VM),
            scratch_shapes=scratch,
            compiler_params=pltpu.CompilerParams(collective_id=1, has_side_effects=True, vmem_limit_bytes=67043328),
            name='whole',
        )(z0, mask, g, ln_pair, w_proj, w_gate, ln_chan, w_out)

        def rows_of(start, count):
            return jnp.swapaxes(grads[:, :, start:start + count], 0, 1).reshape(n * count, c)

        base = 2 * we
        d_wp = jnp.stack([rows_of(we, we).T, rows_of(0, we).T])
        d_wg = jnp.stack([rows_of(base + 3 * wc, wc), rows_of(base, wc)])
        d_wo = jnp.stack([rows_of(base + 2 * wc, wc), rows_of(base + wc, wc)])
        small = small.astype(BF16)
        d_lp = jnp.stack([small[8:10], small[0:2]])
        d_lq = jnp.stack([small[4:6], small[2:4]])
        return z2, dz, d_lp, d_wp, d_wg, d_lq, d_wo

    full = P()
    return jax.shard_map(device_step, mesh=mesh, in_specs=(row_spec, mask_spec, row_spec, full, full, full, full, full), out_specs=(row_spec, row_spec, grad_spec, grad_spec, grad_spec, grad_spec, grad_spec), check_vma=False)
```
